32 devices in a mesh: data: 1 (over z), time: 32 (over y, x, core).
Axes of the slice: x: 4, y: 4, z: 1, core: 2. Of those that a mesh axis runs over, the one named last changes fastest.
The devices are a block of a 4x4x8 slice.
Arguments:
- x_init: float32 [64, 256, 16], P('data')
- w_in: bfloat16 [16, 384], replicated
- w_out: bfloat16 [384, 16], replicated
- mod_scale: bfloat16 [64, 384], P('time')
- mod_shift: bfloat16 [64, 384], P('time')
- step_size: float32 [64], P('time')
Outputs:
- output: float32 [64, 64, 256, 16], P('time', 'data')
All inputs are finite; a program needn't handle non-finite values.
Results may differ from the reference program's by a relative error of at most 0.001.
Values are sent between devices in bfloat16 or wider.
A program may use at most 768 MiB of HBM per device.

```python
import jax
import jax.numpy as jnp
from jax import lax

BATCH = 64
TOKENS = 256
CHANNELS = 16
HIDDEN = 384
STEPS = 64
SWEEPS = 4


def setup_inputs(seed: int = 0, part: int = 0) -> dict:
    key_list = jax.random.split(jax.random.key(seed), 7)
    x_init = jax.random.normal(jax.random.fold_in(key_list[0], part), (BATCH, TOKENS, CHANNELS), jnp.float32)
    w_in = jax.random.normal(key_list[1], (CHANNELS, HIDDEN), jnp.float32) * (CHANNELS * STEPS) ** -0.5
    w_raw = jax.random.normal(key_list[2], (HIDDEN, CHANNELS), jnp.float32)
    w_out = (w_raw - jnp.mean(w_raw, axis=0, keepdims=True)) * (1.5 * HIDDEN ** -0.5)
    time_pos = (jnp.arange(STEPS, dtype=jnp.float32) + 0.5) / STEPS
    mode_coef = 0.4 * jax.random.normal(key_list[3], (3, HIDDEN), jnp.float32)
    mod_scale = (mode_coef[0][None, :] + mode_coef[1][None, :] * jnp.cos(jnp.pi * time_pos)[:, None] + mode_coef[2][None, :] * jnp.cos(2.0 * jnp.pi * time_pos)[:, None] + 0.1 * jax.random.normal(key_list[4], (STEPS, HIDDEN), jnp.float32))
    mod_shift = jax.random.normal(key_list[5], (STEPS, HIDDEN), jnp.float32)
    step_size = jax.random.uniform(key_list[6], (STEPS,), jnp.float32, 0.5, 1.5) * STEPS ** -0.5
    return {"x_init": x_init, "w_in": w_in.astype(jnp.bfloat16), "w_out": w_out.astype(jnp.bfloat16), "mod_scale": mod_scale.astype(jnp.bfloat16), "mod_shift": mod_shift.astype(jnp.bfloat16), "step_size": step_size}


def denoise(latent, w_in, w_out, scale_row, shift_row):
    flat_in = latent.astype(jnp.bfloat16).reshape(-1, latent.shape[-1])
    pre_act = jnp.dot(flat_in, w_in, preferred_element_type=jnp.float32)
    hidden_act = jax.nn.gelu(pre_act * (1.0 + scale_row.astype(jnp.float32)) + shift_row.astype(jnp.float32), approximate=True)
    return jnp.dot(hidden_act.astype(jnp.bfloat16), w_out, preferred_element_type=jnp.float32).reshape(latent.shape)


def reference(x_init, w_in, w_out, mod_scale, mod_shift, step_size):
    def one_step_drift(item):
        return denoise(item[0], w_in, w_out, item[1], item[2])

    def one_sweep(latents, unused):
        drifts = lax.map(one_step_drift, (latents, mod_scale, mod_shift))
        increments = step_size[:-1, None, None, None] * (0.5 * (drifts[:-1] + drifts[1:]))
        running = jnp.cumsum(increments, axis=0)
        return jnp.concatenate([x_init[None], x_init[None] + running], axis=0), unused

    start = jnp.broadcast_to(x_init[None], (STEPS,) + x_init.shape)
    final, unused_out = lax.scan(one_sweep, start, None, length=SWEEPS)
    return final
```

```python
import functools
import math

import jax
import jax.numpy as jnp
from jax import lax
from jax.experimental import pallas as pl
from jax.experimental.pallas import tpu as pltpu
from jax.sharding import PartitionSpec as P

SWEEPS = 4
UNROLL = 8
LANES = 128
C1 = 2.0 * math.sqrt(2.0 / math.pi)
C3 = 8.0 * math.sqrt(2.0 / math.pi) * 0.044715


def compute_kernel(x_ref, scale_ref, shift_ref, w_in_ref, w_out_ref, step_ref, out_ref, w_scr, xs_scr):
    steps = scale_ref.shape[0]
    hidden = scale_ref.shape[1]
    batch, chans, tokens = x_ref.shape
    f32, bf16 = jnp.float32, jnp.bfloat16

    row = lax.broadcasted_iota(jnp.int32, (LANES, LANES), 0)
    lane = lax.broadcasted_iota(jnp.int32, (LANES, LANES), 1)
    eye = (row == lane).astype(f32).astype(bf16)
    mods = jnp.concatenate([scale_ref[...], shift_ref[...]], axis=0)
    tdims = (((0,), (0,)), ((), ()))
    mods_t = lax.dot_general(mods, eye, tdims, preferred_element_type=f32).astype(bf16)
    spread = ((lane % chans == row) & (lane < 3 * chans) & (row < chans)).astype(f32).astype(bf16)
    w3 = 0.5 * lax.dot_general(w_in_ref[...], spread[:chans], tdims, preferred_element_type=f32)
    lane_row = lax.broadcasted_iota(jnp.int32, (1, LANES), 1)
    w3 = w3 + jnp.where(lane_row == 3 * chans, 0.5, 0.0)
    ones = jnp.where(lane_row < 3 * chans, 1.0, 0.0)
    use_hi = (lane_row < chans) | (lane_row >= 3 * chans)
    use_mid = lane_row < 2 * chans

    @pl.loop(0, steps)
    def _(j):
        pick = ((row == j) & (lane < 3 * chans)) | ((row == steps + j) & (lane == 3 * chans))
        picked = jnp.dot(mods_t, pick.astype(f32).astype(bf16), preferred_element_type=f32)
        prod = w3 * (picked + ones)
        hi = prod.astype(bf16).astype(f32)
        rest = prod - hi
        mid = rest.astype(bf16).astype(f32)
        piece = jnp.where(use_hi, hi, jnp.where(use_mid, mid, rest - mid))
        w_scr[j] = piece.astype(bf16)

    w_out_t = w_out_ref[...]
    pad_rows = LANES - 4 * chans
    ones_rows = jnp.ones((chans, tokens), bf16)
    zero_rows = jnp.zeros((pad_rows, tokens), bf16)
    groups = steps // UNROLL

    for b in range(batch):
        x0 = x_ref[b]
        x0_bf = x0.astype(bf16)

        @pl.loop(0, steps)
        def _(j):
            xs_scr[j] = x0_bf

        def body(g, carry):
            d_prev, total = carry
            j0 = lax.rem(g, groups) * UNROLL
            for u in range(UNROLL):
                j = j0 + u
                x = xs_scr[j]
                rhs = jnp.concatenate([x, x, x, ones_rows, zero_rows], axis=0)
                half = jnp.dot(w_scr[j], rhs, preferred_element_type=f32)
                arg = half * (half * half * C3 + C1)
                hid = (half * (1.0 + jnp.tanh(arg))).astype(bf16)
                d = jnp.dot(w_out_t, hid, preferred_element_type=f32)
                if u == 0:
                    inc = step_ref[jnp.maximum(j - 1, 0)] * (0.5 * (d_prev + d))
                    total = jnp.where(j0 == 0, 0.0, total + inc)
                else:
                    total = total + step_ref[j - 1] * (0.5 * (d_prev + d))
                new = x0 + total
                xs_scr[j] = new.astype(bf16)
                out_ref[j, b] = new
                d_prev = d
            return d_prev, total

        zero = jnp.zeros((chans, tokens), f32)
        lax.fori_loop(0, SWEEPS * groups, body, (zero, zero))


def solution(mesh):
    n_time = mesh.shape["time"]

    def local(x_init, w_in, w_out, mod_scale, mod_shift, step_size):
        batch, tokens, chans = x_init.shape
        hidden = w_in.shape[1]
        share = batch // n_time
        me = lax.axis_index("time")
        scale = lax.all_gather(mod_scale, "time", tiled=True)
        shift = lax.all_gather(mod_shift, "time", tiled=True)
        step = lax.all_gather(step_size, "time", tiled=True)
        steps = scale.shape[0]
        x_t = jnp.swapaxes(x_init, 1, 2)
        x_mine = lax.dynamic_slice_in_dim(x_t, me * share, share, 0)
        vmem = pl.BlockSpec(memory_space=pltpu.VMEM)
        out = pl.pallas_call(
            compute_kernel,
            out_shape=jax.ShapeDtypeStruct((steps, share, chans, tokens), jnp.float32),
            in_specs=[vmem] * 5 + [pl.BlockSpec(memory_space=pltpu.SMEM)],
            out_specs=vmem,
            scratch_shapes=[
                pltpu.VMEM((steps, hidden, LANES), jnp.bfloat16),
                pltpu.VMEM((steps, chans, tokens), jnp.bfloat16),
            ],
            compiler_params=pltpu.CompilerParams(vmem_limit_bytes=48 * 1024 * 1024),
            name="sweeps",
        )(x_mine, scale, shift, w_in, w_out.T, step)
        out = lax.all_to_all(out, "time", split_axis=0, concat_axis=1, tiled=True)
        return jnp.swapaxes(out, 2, 3)

    return jax.shard_map(local, mesh=mesh, in_specs=(P("data"), P(), P(), P("time"), P("time"), P("time")), out_specs=P("time", "data"), check_vma=False)
```

```python
import functools
import math

import jax
import jax.numpy as jnp
from jax import lax
from jax.experimental import pallas as pl
from jax.experimental.pallas import tpu as pltpu
from jax.sharding import PartitionSpec as P

SWEEPS = 4
UNROLL = 16
AHEAD = 2
LANES = 128
FOLD_LIMIT = 2.0 ** 60
C1 = 2.0 * math.sqrt(2.0 / math.pi)
C3 = 8.0 * math.sqrt(2.0 / math.pi) * 0.044715
F32, BF16 = jnp.float32, jnp.bfloat16
MESH = pl.DeviceIdType.MESH
CONTRACT0 = (((0,), (0,)), ((), ()))


def signal_all(n, me):
    barrier = pltpu.get_barrier_semaphore()

    @pl.loop(1, n)
    def _(i):
        pl.semaphore_signal(barrier, inc=1, device_id={"time": lax.rem(me + i, n)}, device_id_type=MESH)


def one_hot(cond):
    return jnp.where(cond, 1.0, 0.0).astype(BF16)


def gather_kernel(n, scale_ref, shift_ref, step_ref, w_in_ref, mods_t_ref, steps_ref, flag_ref, mine, mine_step, mods, send_sem, recv_sem):
    me = lax.axis_index("time")
    signal_all(n, me)
    per = scale_ref.shape[0]
    mine[0:per] = scale_ref[...]
    mine[per:2 * per] = shift_ref[...]
    lane = lax.broadcasted_iota(jnp.int32, (1, LANES), 1)
    row = jnp.zeros((1, LANES), F32)
    for i in range(per):
        row = jnp.where(lane == i, step_ref[i], row)
    mine_step[...] = row
    pl.semaphore_wait(pltpu.get_barrier_semaphore(), n - 1)

    def copies(i):
        to = {"time": lax.rem(me + i, n)}
        return (
            pltpu.make_async_remote_copy(mine, mods.at[me], send_sem.at[0, i], recv_sem.at[0, i], device_id=to, device_id_type=MESH),
            pltpu.make_async_remote_copy(mine_step, steps_ref.at[me], send_sem.at[1, i], recv_sem.at[1, i], device_id=to, device_id_type=MESH),
        )

    @pl.loop(1, n)
    def _(i):
        for c in copies(i):
            c.start()

    mods[me] = mine[...]
    steps_ref[me] = mine_step[...]

    @pl.loop(1, n)
    def _(i):
        for c in copies(i):
            c.wait()

    parts = [mods[q].astype(F32) for q in range(n)]
    flat = jnp.concatenate(parts, axis=0).astype(BF16)
    r = lax.broadcasted_iota(jnp.int32, (LANES, LANES), 0)
    c = lax.broadcasted_iota(jnp.int32, (LANES, LANES), 1)
    mods_t_ref[...] = lax.dot_general(flat, one_hot(r == c), CONTRACT0, preferred_element_type=F32).astype(BF16)
    top = 0.0
    for q in range(n):
        top = jnp.maximum(top, jnp.abs(1.0 + parts[q][:per]))
    bound = jnp.max(top) * jnp.max(jnp.abs(w_in_ref[...].astype(F32)))
    flag_ref[0] = (bound <= FOLD_LIMIT).astype(jnp.int32)


def scale_row(j, per):
    return j // per * (2 * per) + lax.rem(j, per)


def sweeps_kernel(n, per, fold, x_ref, mods_t_ref, w_in_ref, w_out_ref, step_ref, out_ref, w_scr, xs_scr, res_scr, send_sem, recv_sem):
    me = lax.axis_index("time")
    signal_all(n, me)
    share, chans, tokens = x_ref.shape
    steps = n * per
    mods_t = mods_t_ref[...]

    row = lax.broadcasted_iota(jnp.int32, (LANES, LANES), 0)
    lane = lax.broadcasted_iota(jnp.int32, (LANES, LANES), 1)
    lane_row = lax.broadcasted_iota(jnp.int32, (1, LANES), 1)
    spread = one_hot((lane % chans == row) & (lane < 3 * chans))
    w3 = 0.5 * lax.dot_general(w_in_ref[...], spread[:chans], CONTRACT0, preferred_element_type=F32)

    if fold:
        w3 = w3 + jnp.where(lane_row == 3 * chans, 0.5, 0.0)
        ones = jnp.where(lane_row < 3 * chans, 1.0, 0.0)
        use_hi = (lane_row < chans) | (lane_row >= 3 * chans)
        use_mid = lane_row < 2 * chans

        @pl.loop(0, steps)
        def _(j):
            src = scale_row(j, per)
            pick = ((row == src) & (lane < 3 * chans)) | ((row == src + per) & (lane == 3 * chans))
            picked = jnp.dot(mods_t, one_hot(pick), preferred_element_type=F32)
            prod = w3 * (picked + ones)
            hi = prod.astype(BF16).astype(F32)
            rest = prod - hi
            mid = rest.astype(BF16).astype(F32)
            w_scr[j] = jnp.where(use_hi, hi, jnp.where(use_mid, mid, rest - mid)).astype(BF16)
    else:
        w_scr[0] = (w3 * jnp.where(lane_row < chans, 2.0, 0.0)).astype(BF16)

    w_out_t = w_out_ref[...]
    ones_rows = jnp.ones((chans, tokens), BF16)
    zero_rows = jnp.zeros((LANES - 4 * chans, tokens), BF16)
    row_tok = lax.broadcasted_iota(jnp.int32, (LANES, tokens), 0)
    unroll = UNROLL if fold else per
    groups = steps // unroll

    def half_pre(j, x):
        rhs = jnp.concatenate([x, x, x, ones_rows, zero_rows], axis=0)
        if fold:
            return jnp.dot(w_scr[j], rhs, preferred_element_type=F32)
        u = jnp.dot(w_scr[0], rhs, preferred_element_type=F32)
        src = scale_row(j, per)
        scale = jnp.dot(mods_t, one_hot(row_tok == src), preferred_element_type=F32)
        shift = jnp.dot(mods_t, one_hot(row_tok == src + per), preferred_element_type=F32)
        return 0.5 * (u * (1.0 + scale) + shift)

    def copy(b, i):
        q = lax.rem(me + i, n)
        return pltpu.make_async_remote_copy(
            res_scr.at[pl.ds(q * per, per), b], out_ref.at[:, me * share + b], send_sem.at[b, i], recv_sem.at[b, i],
            device_id={"time": q}, device_id_type=MESH)

    for b in range(share):
        x0 = x_ref[b]
        x0_bf = x0.astype(BF16)

        @pl.loop(0, steps)
        def _(j):
            xs_scr[j] = x0_bf

        def body(g, carry):
            d_prev, total = carry
            j0 = lax.rem(g, groups) * unroll
            xs = [xs_scr[j0 + u] for u in range(unroll)]
            halves, ds = {}, []
            for u in range(unroll + AHEAD):
                if u < unroll:
                    halves[u] = half_pre(j0 + u, xs[u])
                if u >= AHEAD:
                    half = halves.pop(u - AHEAD)
                    arg = half * (half * half * C3 + C1)
                    hidden = (half * (1.0 + jnp.tanh(arg))).astype(BF16)
                    ds.append(jnp.dot(w_out_t, hidden, preferred_element_type=F32))
            for u in range(unroll):
                j = j0 + u
                d = ds[u]
                i = jnp.maximum(j - 1, 0)
                inc = step_ref[i // per, 0, lax.rem(i, per)] * (0.5 * (d_prev + d))
                total = total + inc
                if u == 0:
                    total = jnp.where(j0 == 0, 0.0, total)
                new = x0 + total
                xs_scr[j] = new.astype(BF16)
                res_scr[j, b] = new
                d_prev = d
            return d_prev, total

        zero = jnp.zeros((chans, tokens), F32)
        lax.fori_loop(0, SWEEPS * groups, body, (zero, zero))
        if b == 0:
            pl.semaphore_wait(pltpu.get_barrier_semaphore(), n - 1)

        @pl.loop(1, n)
        def _(i):
            copy(b, i).start()

        out_ref[:, me * share + b] = res_scr[pl.ds(me * per, per), b]

    for b in range(share):
        @pl.loop(1, n)
        def _(i):
            copy(b, i).wait()


def solution(mesh):
    n = mesh.shape["time"]
    vmem = pl.BlockSpec(memory_space=pltpu.VMEM)
    smem = pl.BlockSpec(memory_space=pltpu.SMEM)

    def local(x_init, w_in, w_out, mod_scale, mod_shift, step_size):
        batch, tokens, chans = x_init.shape
        per, hidden = mod_scale.shape
        share = batch // n
        me = lax.axis_index("time")
        x_mine = lax.dynamic_slice_in_dim(jnp.swapaxes(x_init, 1, 2), me * share, share, 0)
        mods_t, steps, flag = pl.pallas_call(
            functools.partial(gather_kernel, n),
            out_shape=(
                jax.ShapeDtypeStruct((hidden, LANES), BF16),
                jax.ShapeDtypeStruct((n, 1, LANES), F32),
                jax.ShapeDtypeStruct((1,), jnp.int32),
            ),
            in_specs=[vmem, vmem, smem, vmem],
            out_specs=(vmem, vmem, smem),
            scratch_shapes=[
                pltpu.VMEM((2 * per, hidden), BF16),
                pltpu.VMEM((1, LANES), F32),
                pltpu.VMEM((n, 2 * per, hidden), BF16),
                pltpu.SemaphoreType.DMA((2, n)),
                pltpu.SemaphoreType.DMA((2, n)),
            ],
            compiler_params=pltpu.CompilerParams(collective_id=0, has_side_effects=True),
            name="gather",
        )(mod_scale, mod_shift, step_size, w_in)

        def sweeps(fold, *operands):
            return pl.pallas_call(
                functools.partial(sweeps_kernel, n, per, fold),
                out_shape=jax.ShapeDtypeStruct((per, batch, chans, tokens), F32),
                in_specs=[vmem] * 4 + [smem],
                out_specs=vmem,
                scratch_shapes=[
                    pltpu.VMEM((n * per if fold else 1, hidden, LANES), BF16),
                    pltpu.VMEM((n * per, chans, tokens), BF16),
                    pltpu.VMEM((n * per, share, chans, tokens), F32),
                    pltpu.SemaphoreType.DMA((share, n)),
                    pltpu.SemaphoreType.DMA((share, n)),
                ],
                compiler_params=pltpu.CompilerParams(
                    collective_id=1 if fold else 2, has_side_effects=True, vmem_limit_bytes=40 * 1024 * 1024),
                name="sweeps" if fold else "sweeps_wide",
            )(*operands)

        out = lax.cond(
            flag[0] != 0, functools.partial(sweeps, True), functools.partial(sweeps, False),
            x_mine, mods_t, w_in, w_out.T, steps)
        return jnp.swapaxes(out, 2, 3)

    return jax.shard_map(local, mesh=mesh, in_specs=(P("data"), P(), P(), P("time"), P("time"), P("time")), out_specs=P("time", "data"), check_vma=False)
```

```python
import functools
import math

import jax
import jax.numpy as jnp
from jax import lax
from jax.experimental import pallas as pl
from jax.experimental.pallas import tpu as pltpu
from jax.sharding import PartitionSpec as P

SWEEPS = 4
UNROLL = 16
PICKS = 4
EARLY = 9
AHEAD = 2
LANES = 128
FOLD_LIMIT = 2.0 ** 60
C1 = 2.0 * math.sqrt(2.0 / math.pi)
C3 = 8.0 * math.sqrt(2.0 / math.pi) * 0.044715
F32, BF16 = jnp.float32, jnp.bfloat16
MESH = pl.DeviceIdType.MESH
CONTRACT0 = (((0,), (0,)), ((), ()))


def signal_all(n, me):
    barrier = pltpu.get_barrier_semaphore()

    @pl.loop(1, n)
    def _(i):
        pl.semaphore_signal(barrier, inc=1, device_id={"time": lax.rem(me + i, n)}, device_id_type=MESH)


def one_hot(cond):
    return jnp.where(cond, 1.0, 0.0).astype(BF16)


def gather_kernel(n, scale_ref, shift_ref, step_ref, w_in_ref, mods_t_ref, steps_ref, flag_ref, mine, mine_step, mods, send_sem, recv_sem):
    me = lax.axis_index("time")
    signal_all(n, me)
    per = scale_ref.shape[0]
    mine[0:per] = scale_ref[...]
    mine[per:2 * per] = shift_ref[...]
    lane = lax.broadcasted_iota(jnp.int32, (1, LANES), 1)
    row = jnp.zeros((1, LANES), F32)
    for i in range(per):
        row = jnp.where(lane == i, step_ref[i], row)
    mine_step[...] = row
    pl.semaphore_wait(pltpu.get_barrier_semaphore(), n - 1)

    def copies(i):
        to = {"time": lax.rem(me + i, n)}
        return (
            pltpu.make_async_remote_copy(mine, mods.at[me], send_sem.at[0, i], recv_sem.at[0, i], device_id=to, device_id_type=MESH),
            pltpu.make_async_remote_copy(mine_step, steps_ref.at[me], send_sem.at[1, i], recv_sem.at[1, i], device_id=to, device_id_type=MESH),
        )

    @pl.loop(1, n)
    def _(i):
        for c in copies(i):
            c.start()

    mods[me] = mine[...]
    steps_ref[me] = mine_step[...]

    @pl.loop(1, n)
    def _(i):
        for c in copies(i):
            c.wait()

    parts = [mods[q].astype(F32) for q in range(n)]
    flat = jnp.concatenate(parts, axis=0).astype(BF16)
    r = lax.broadcasted_iota(jnp.int32, (LANES, LANES), 0)
    c = lax.broadcasted_iota(jnp.int32, (LANES, LANES), 1)
    mods_t_ref[...] = lax.dot_general(flat, one_hot(r == c), CONTRACT0, preferred_element_type=F32).astype(BF16)
    top = 0.0
    for q in range(n):
        top = jnp.maximum(top, jnp.abs(1.0 + parts[q][:per]))
    bound = jnp.max(top) * jnp.max(jnp.abs(w_in_ref[...].astype(F32)))
    flag_ref[0] = (bound <= FOLD_LIMIT).astype(jnp.int32)


def scale_row(j, per):
    return j // per * (2 * per) + lax.rem(j, per)


def sweeps_kernel(n, per, fold, x_hbm, mods_t_ref, w_in_ref, w_out_ref, step_ref, out_ref, x_scr, w_scr, xs_scr, z_scr, h_scr, res_scr, x_sem, send_sem, recv_sem):
    me = lax.axis_index("time")
    signal_all(n, me)
    share, chans, tokens = x_scr.shape
    steps = n * per
    half_lanes = LANES // 2
    load_x = pltpu.make_async_copy(x_hbm.at[pl.ds(me * share, share)], x_scr, x_sem)
    load_x.start()
    mods_t = mods_t_ref[...]

    row = lax.broadcasted_iota(jnp.int32, (LANES, LANES), 0)
    lane = lax.broadcasted_iota(jnp.int32, (1, LANES), 1)
    slot = lax.rem(lane, half_lanes)
    spread = one_hot((lax.rem(lane, chans) == row) & (slot < 3 * chans))
    w3 = 0.5 * lax.dot_general(w_in_ref[...], spread[:chans], CONTRACT0, preferred_element_type=F32)

    if fold:
        w3 = w3 + jnp.where(slot == 3 * chans, 0.5, 0.0)
        ones = jnp.where(slot < 3 * chans, 1.0, 0.0)
        rest_lanes = (slot >= chans) & (slot < 3 * chans)
        low_lanes = (slot >= 2 * chans) & (slot < 3 * chans)
        wide_row = lax.broadcasted_iota(jnp.int32, (LANES, 2 * LANES), 0)
        wide_lane = lax.broadcasted_iota(jnp.int32, (1, 2 * LANES), 1)
        wide_slot = lax.rem(wide_lane, half_lanes)
        source = scale_row(wide_lane // half_lanes, per) + jnp.where(wide_slot == 3 * chans, per, 0)
        source = jnp.where(wide_slot <= 3 * chans, source, -8 * steps)
        ahead = wide_row - source

        def build(g, unused):
            picked = []
            for t in range(PICKS):
                first = (g * PICKS + t) * 8
                picked.append(jnp.dot(mods_t, one_hot(ahead == first), preferred_element_type=F32))
            for t in range(PICKS):
                for p in range(2):
                    prod = w3 * (picked[t][:, p * LANES:(p + 1) * LANES] + ones)
                    rest = prod - jnp.where(rest_lanes, prod.astype(BF16).astype(F32), 0.0)
                    rest = rest - jnp.where(low_lanes, rest.astype(BF16).astype(F32), 0.0)
                    w_scr[(g * PICKS + t) * 2 + p] = rest.astype(BF16)
            return unused

        lax.fori_loop(0, steps // (4 * PICKS), build, 0)
    else:
        w_scr[0] = (w3 * jnp.where(lane < chans, 2.0, 0.0)).astype(BF16)

    w_out_t = w_out_ref[...]
    ones_rows = jnp.ones((chans, tokens), BF16)
    zero_rows = jnp.zeros((half_lanes, tokens), BF16)
    row_tok = lax.broadcasted_iota(jnp.int32, (LANES, tokens), 0)
    unroll = UNROLL if fold else 2 * AHEAD
    groups = steps // unroll
    early = max(unroll - EARLY, 0)

    def half_pre(j0, u, x):
        parts = [x, x, x, ones_rows]
        if fold:
            rhs = jnp.concatenate(parts + [zero_rows] if u % 2 == 0 else [zero_rows] + parts, axis=0)
            return jnp.dot(w_scr[j0 // 2 + u // 2], rhs, preferred_element_type=F32)
        pre = jnp.dot(w_scr[0], jnp.concatenate(parts + [zero_rows], axis=0), preferred_element_type=F32)
        src = scale_row(j0 + u, per)
        scale = jnp.dot(mods_t, one_hot(row_tok == src), preferred_element_type=F32)
        shift = jnp.dot(mods_t, one_hot(row_tok == src + per), preferred_element_type=F32)
        return 0.5 * (pre * (1.0 + scale) + shift)

    def project(hidden):
        return jnp.dot(w_out_t, hidden, preferred_element_type=F32)

    def copy(b, i):
        q = lax.rem(me + i, n)
        return pltpu.make_async_remote_copy(
            res_scr.at[pl.ds(q * per, per), b], out_ref.at[:, me * share + b], send_sem.at[b, i], recv_sem.at[b, i],
            device_id={"time": q}, device_id_type=MESH)

    load_x.wait()
    for b in range(share):
        x0 = x_scr[b]
        x0_bf = x0.astype(BF16)

        @pl.loop(0, steps)
        def _(j):
            xs_scr[j] = x0_bf

        def advance(j, d, d_prev, total, first=None):
            i = jnp.maximum(j - 1, 0)
            total = total + step_ref[i // per, 0, lax.rem(i, per)] * (0.5 * (d_prev + d))
            if first is not None:
                total = jnp.where(first, 0.0, total)
            new = x0 + total
            xs_scr[j] = new.astype(BF16)
            res_scr[j, b] = new
            return d, total

        def body(g, carry):
            j0 = lax.rem(g, groups) * unroll
            j_next = lax.rem(g + 1, groups) * unroll
            xs = [xs_scr[j0 + u] for u in range(AHEAD, unroll)] + [xs_scr[j_next + u] for u in range(AHEAD)]
            ds = [project(h_scr[...])]
            halves = {u: z_scr[u] for u in range(AHEAD)}
            for u in range(unroll):
                v = u + AHEAD
                if v < unroll:
                    halves[v] = half_pre(j0, v, xs[u])
                half = halves.pop(u)
                arg = half * (half * half * C3 + C1)
                hidden = (half * (1.0 + jnp.tanh(arg))).astype(BF16)
                if early <= u < early + AHEAD:
                    z_scr[u - early] = half_pre(j_next, u - early, xs[u - early - AHEAD])
                if u < unroll - 1:
                    ds.append(project(hidden))
                else:
                    h_scr[...] = hidden
            carry = advance(lax.rem(j0 + steps - 1, steps), ds[0], *carry)
            for u in range(unroll - 1):
                carry = advance(j0 + u, ds[u + 1], *carry, first=j0 == 0 if u == 0 else None)
            return carry

        for u in range(AHEAD):
            z_scr[u] = half_pre(0, u, x0_bf)
        h_scr[...] = jnp.zeros_like(h_scr)
        zero = jnp.zeros((chans, tokens), F32)
        carry = lax.fori_loop(0, SWEEPS * groups, body, (zero, zero))
        advance(steps - 1, project(h_scr[...]), *carry)
        if b == 0:
            pl.semaphore_wait(pltpu.get_barrier_semaphore(), n - 1)

        @pl.loop(1, n)
        def _(i):
            copy(b, i).start()

        out_ref[:, me * share + b] = res_scr[pl.ds(me * per, per), b]

    for b in range(share):
        @pl.loop(1, n)
        def _(i):
            copy(b, i).wait()


def solution(mesh):
    n = mesh.shape["time"]
    vmem = pl.BlockSpec(memory_space=pltpu.VMEM)
    smem = pl.BlockSpec(memory_space=pltpu.SMEM)

    def local(x_init, w_in, w_out, mod_scale, mod_shift, step_size):
        batch, tokens, chans = x_init.shape
        per, hidden = mod_scale.shape
        share = batch // n
        mods_t, steps, flag = pl.pallas_call(
            functools.partial(gather_kernel, n),
            out_shape=(
                jax.ShapeDtypeStruct((hidden, LANES), BF16),
                jax.ShapeDtypeStruct((n, 1, LANES), F32),
                jax.ShapeDtypeStruct((1,), jnp.int32),
            ),
            in_specs=[vmem, vmem, smem, vmem],
            out_specs=(vmem, vmem, smem),
            scratch_shapes=[
                pltpu.VMEM((2 * per, hidden), BF16),
                pltpu.VMEM((1, LANES), F32),
                pltpu.VMEM((n, 2 * per, hidden), BF16),
                pltpu.SemaphoreType.DMA((2, n)),
                pltpu.SemaphoreType.DMA((2, n)),
            ],
            compiler_params=pltpu.CompilerParams(collective_id=0, has_side_effects=True),
            name="gather",
        )(mod_scale, mod_shift, step_size, w_in)

        def sweeps(fold, *operands):
            return pl.pallas_call(
                functools.partial(sweeps_kernel, n, per, fold),
                out_shape=jax.ShapeDtypeStruct((per, batch, chans, tokens), F32),
                in_specs=[pl.BlockSpec(memory_space=pl.ANY)] + [vmem] * 3 + [smem],
                out_specs=vmem,
                scratch_shapes=[
                    pltpu.VMEM((share, chans, tokens), F32),
                    pltpu.VMEM((n * per // 2 if fold else 1, hidden, LANES), BF16),
                    pltpu.VMEM((n * per, chans, tokens), BF16),
                    pltpu.VMEM((AHEAD, hidden, tokens), F32),
                    pltpu.VMEM((hidden, tokens), BF16),
                    pltpu.VMEM((n * per, share, chans, tokens), F32),
                    pltpu.SemaphoreType.DMA,
                    pltpu.SemaphoreType.DMA((share, n)),
                    pltpu.SemaphoreType.DMA((share, n)),
                ],
                compiler_params=pltpu.CompilerParams(
                    collective_id=1 if fold else 2, has_side_effects=True, vmem_limit_bytes=40 * 1024 * 1024),
                name="sweeps" if fold else "sweeps_wide",
            )(*operands)

        out = lax.cond(
            flag[0] != 0, functools.partial(sweeps, True), functools.partial(sweeps, False),
            jnp.swapaxes(x_init, 1, 2), mods_t, w_in, w_out.T, steps)
        return jnp.swapaxes(out, 2, 3)

    return jax.shard_map(local, mesh=mesh, in_specs=(P("data"), P(), P(), P("time"), P("time"), P("time")), out_specs=P("time", "data"), check_vma=False)
```

```python
import functools
import math

import jax
import jax.numpy as jnp
from jax import lax
from jax.experimental import pallas as pl
from jax.experimental.pallas import tpu as pltpu
from jax.sharding import PartitionSpec as P

SWEEPS = 4
UNROLL = 16
PICKS = 4
EARLY = 9
AHEAD = 2
LANES = 128
WIDTH = 128
FOLD_LIMIT = 2.0 ** 60
C1 = 2.0 * math.sqrt(2.0 / math.pi)
C3 = 8.0 * math.sqrt(2.0 / math.pi) * 0.044715
F32, BF16 = jnp.float32, jnp.bfloat16
MESH = pl.DeviceIdType.MESH
CONTRACT0 = (((0,), (0,)), ((), ()))


def offsets(n):
    return sorted(range(1, n), key=lambda i: (abs(2 * i - n), i))


def signal_all(n, me):
    barrier = pltpu.get_barrier_semaphore()
    for i in offsets(n):
        pl.semaphore_signal(barrier, inc=1, device_id={"time": lax.rem(me + i, n)}, device_id_type=MESH)


def wait_bytes(ref, *sems):
    for sem in sems:
        pltpu.make_async_copy(ref, ref, sem).wait()


def one_hot(cond):
    return jnp.where(cond, 1.0, 0.0).astype(BF16)


def gather_kernel(n, scale_hbm, shift_hbm, step_hbm, w_in_hbm, mods_t_ref, steps_ref, flag_ref, scale, shift, step, w_in, mine, mine_step, mods, load_sem, send_sem, recv_sem):
    me = lax.axis_index("time")
    loads = [
        pltpu.make_async_copy(src, dst, load_sem.at[k])
        for k, (src, dst) in enumerate(((scale_hbm, scale), (shift_hbm, shift), (step_hbm, step), (w_in_hbm, w_in)))
    ]
    for load in loads:
        load.start()
    signal_all(n, me)
    for load in loads:
        load.wait()
    per = scale.shape[0]
    mine[0:per] = scale[...]
    mine[per:2 * per] = shift[...]
    lane = lax.broadcasted_iota(jnp.int32, (1, LANES), 1)
    row = jnp.zeros((1, LANES), F32)
    for i in range(per):
        row = jnp.where(lane == i, step[i], row)
    mine_step[...] = row
    mods[me] = mine[...]
    steps_ref[me] = mine_step[...]
    w_top = jnp.max(jnp.abs(w_in[...].astype(F32)))
    pl.semaphore_wait(pltpu.get_barrier_semaphore(), n - 1)

    for i in offsets(n):
        to = {"time": lax.rem(me + i, n)}
        pltpu.make_async_remote_copy(mine, mods.at[me], send_sem.at[0], recv_sem.at[0], device_id=to, device_id_type=MESH).start()
        pltpu.make_async_remote_copy(mine_step, steps_ref.at[me], send_sem.at[1], recv_sem.at[1], device_id=to, device_id_type=MESH).start()
    wait_bytes(mods.at[pl.ds(0, n - 1)], recv_sem.at[0])

    parts = [mods[q].astype(F32) for q in range(n)]
    flat = jnp.concatenate(parts, axis=0).astype(BF16)
    r = lax.broadcasted_iota(jnp.int32, (LANES, LANES), 0)
    c = lax.broadcasted_iota(jnp.int32, (LANES, LANES), 1)
    mods_t_ref[...] = lax.dot_general(flat, one_hot(r == c), CONTRACT0, preferred_element_type=F32).astype(BF16)
    top = 0.0
    for q in range(n):
        top = jnp.maximum(top, jnp.abs(1.0 + parts[q][:per]))
    flag_ref[0] = (jnp.max(top) * w_top <= FOLD_LIMIT).astype(jnp.int32)
    wait_bytes(steps_ref.at[pl.ds(0, n - 1)], recv_sem.at[1], send_sem.at[1])
    wait_bytes(mods.at[pl.ds(0, n - 1)], send_sem.at[0])


def scale_row(j, per):
    return j // per * (2 * per) + lax.rem(j, per)


def sweeps_kernel(n, per, fold, x_hbm, mods_t_ref, w_in_ref, w_out_ref, step_ref, out_ref, x_scr, w_scr, xs_scr, z_scr, h_scr, res_scr, x_sem, send_sem, recv_sem):
    me = lax.axis_index("time")
    chunks, chans, width = x_scr.shape
    tokens = x_hbm.shape[2]
    cuts = tokens // width
    share = chunks // cuts
    steps = n * per
    tiles = steps // 2
    half_lanes = LANES // 2

    def x_copy(c):
        return pltpu.make_async_copy(x_hbm.at[me * share + c // cuts, :, pl.ds(c % cuts * width, width)], x_scr.at[c], x_sem.at[c])

    for c in range(chunks):
        x_copy(c).start()
    signal_all(n, me)
    mods_t = mods_t_ref[...]

    row = lax.broadcasted_iota(jnp.int32, (LANES, LANES), 0)
    lane = lax.broadcasted_iota(jnp.int32, (1, LANES), 1)
    slot = lax.rem(lane, half_lanes)
    spread = one_hot((lax.rem(lane, chans) == row) & (slot < 3 * chans))
    w3 = 0.5 * lax.dot_general(w_in_ref[...], spread[:chans], CONTRACT0, preferred_element_type=F32)
    wide_row = lax.broadcasted_iota(jnp.int32, (LANES, 2 * LANES), 0)
    wide_lane = lax.broadcasted_iota(jnp.int32, (1, 2 * LANES), 1)

    if fold:
        w3 = w3 + jnp.where(slot == 3 * chans, 0.5, 0.0)
        ones = jnp.where(slot < 3 * chans, 1.0, 0.0)
        rest_lanes = (slot >= chans) & (slot < 3 * chans)
        low_lanes = (slot >= 2 * chans) & (slot < 3 * chans)
        wide_slot = lax.rem(wide_lane, half_lanes)
        source = scale_row(wide_lane // half_lanes, per) + jnp.where(wide_slot == 3 * chans, per, 0)
        source = jnp.where(wide_slot <= 3 * chans, source, -8 * steps)
        ahead = wide_row - source

        def build(g, unused):
            picked = []
            for t in range(PICKS):
                first = (g * PICKS + t) * 8
                picked.append(jnp.dot(mods_t, one_hot(ahead == first), preferred_element_type=F32))
            for t in range(PICKS):
                for p in range(2):
                    prod = w3 * (picked[t][:, p * LANES:(p + 1) * LANES] + ones)
                    rest = prod - jnp.where(rest_lanes, prod.astype(BF16).astype(F32), 0.0)
                    rest = rest - jnp.where(low_lanes, rest.astype(BF16).astype(F32), 0.0)
                    w_scr[(g * PICKS + t) * 2 + p] = rest.astype(BF16)
            return unused

        lax.fori_loop(0, steps // (4 * PICKS), build, 0)
    else:
        w_scr[0] = (w3 * jnp.where(lane < chans, 2.0, 0.0)).astype(BF16)

    w_out_t = w_out_ref[...]
    ones_rows = jnp.ones((chans, width), BF16)
    zero_rows = jnp.zeros((half_lanes, width), BF16)
    unroll = UNROLL if fold else 2 * AHEAD
    groups = tiles // unroll
    per_chunk = SWEEPS * groups
    early = max(unroll - EARLY, 0)

    def half_pre(t, x):
        tops = [jnp.concatenate([x[p], x[p], x[p], ones_rows], axis=0) for p in range(2)]
        if fold:
            left = jnp.concatenate([tops[0], zero_rows], axis=0)
            right = jnp.concatenate([zero_rows, tops[1]], axis=0)
            return jnp.dot(w_scr[t], jnp.concatenate([left, right], axis=1), preferred_element_type=F32)
        rhs = jnp.concatenate([jnp.concatenate([top, zero_rows], axis=0) for top in tops], axis=1)
        pre = jnp.dot(w_scr[0], rhs, preferred_element_type=F32)
        src = scale_row(2 * t + wide_lane // width, per)
        scale = jnp.dot(mods_t, one_hot(wide_row == src), preferred_element_type=F32)
        shift = jnp.dot(mods_t, one_hot(wide_row == src + per), preferred_element_type=F32)
        return 0.5 * (pre * (1.0 + scale) + shift)

    def project(hidden):
        return jnp.dot(w_out_t, hidden, preferred_element_type=F32)

    def load_xs(t):
        return xs_scr[2 * t], xs_scr[2 * t + 1]

    def advance(g, t, d, d_prev, total, first=None):
        c = jnp.maximum(g, 0) // per_chunk
        x0 = x_scr[c]
        x_next = x_scr[jnp.minimum((g + per_chunk) // per_chunk, chunks - 1)]
        last = lax.rem(g + per_chunk, per_chunk) >= per_chunk - groups
        for p in range(2):
            j = 2 * t + p
            i = jnp.maximum(j - 1, 0)
            part = d[:, p * width:(p + 1) * width]
            total = total + step_ref[i // per, 0, lax.rem(i, per)] * (0.5 * (d_prev + part))
            if p == 0 and first is not None:
                total = jnp.where(first, 0.0, total)
            new = x0 + total
            xs_scr[j] = jnp.where(last, x_next, new).astype(BF16)
            res_scr[j, c] = new
            d_prev = part
        return d_prev, total

    def send(c):
        place = (slice(None), me * share + c // cuts, slice(None), pl.ds(pl.multiple_of(lax.rem(c, cuts) * width, width), width))
        for i in offsets(n):
            q = lax.rem(me + i, n)
            pltpu.make_async_remote_copy(
                res_scr.at[pl.ds(q * per, per), c], out_ref.at[place], send_sem, recv_sem,
                device_id={"time": q}, device_id_type=MESH).start()
        out_ref[place] = res_scr[pl.ds(me * per, per), c]

    def body(g, carry):
        t0 = lax.rem(g, groups) * unroll
        t_next = lax.rem(g + 1, groups) * unroll
        xs = [load_xs(t0 + u) for u in range(AHEAD, unroll)] + [load_xs(t_next + u) for u in range(AHEAD)]
        ds = [project(h_scr[...])]
        halves = {u: z_scr[u] for u in range(AHEAD)}
        for u in range(unroll):
            v = u + AHEAD
            if v < unroll:
                halves[v] = half_pre(t0 + v, xs[u])
            half = halves.pop(u)
            arg = half * (half * half * C3 + C1)
            hidden = (half * (1.0 + jnp.tanh(arg))).astype(BF16)
            if early <= u < early + AHEAD:
                z_scr[u - early] = half_pre(t_next + u - early, xs[u - early - AHEAD])
            if u < unroll - 1:
                ds.append(project(hidden))
            else:
                h_scr[...] = hidden
        carry = advance(g - 1, lax.rem(t0 + tiles - 1, tiles), ds[0], *carry)
        for u in range(unroll - 1):
            carry = advance(g, t0 + u, ds[u + 1], *carry, first=t0 == 0 if u == 0 else None)

        @pl.when((g > 0) & (lax.rem(g, per_chunk) == 0))
        def _():
            send(g // per_chunk - 1)

        return carry

    for c in range(chunks):
        x_copy(c).wait()
    x_first = x_scr[0].astype(BF16)

    @pl.loop(0, steps)
    def _(j):
        xs_scr[j] = x_first

    for u in range(AHEAD):
        z_scr[u] = half_pre(u, (x_first, x_first))
    h_scr[...] = jnp.zeros_like(h_scr)
    pl.semaphore_wait(pltpu.get_barrier_semaphore(), n - 1)
    zero = jnp.zeros((chans, width), F32)
    total_groups = chunks * per_chunk
    carry = lax.fori_loop(0, total_groups, body, (zero, zero))
    advance(total_groups - 1, tiles - 1, project(h_scr[...]), *carry)
    send(chunks - 1)
    wait_bytes(res_scr.at[pl.ds(0, (n - 1) * per)], recv_sem, send_sem)


def solution(mesh):
    n = mesh.shape["time"]
    vmem = pl.BlockSpec(memory_space=pltpu.VMEM)
    smem = pl.BlockSpec(memory_space=pltpu.SMEM)

    def local(x_init, w_in, w_out, mod_scale, mod_shift, step_size):
        batch, tokens, chans = x_init.shape
        per, hidden = mod_scale.shape
        share = batch // n
        any_spec = pl.BlockSpec(memory_space=pl.ANY)
        mods_t, steps, flag = pl.pallas_call(
            functools.partial(gather_kernel, n),
            out_shape=(
                jax.ShapeDtypeStruct((hidden, LANES), BF16),
                jax.ShapeDtypeStruct((n, 1, LANES), F32),
                jax.ShapeDtypeStruct((1,), jnp.int32),
            ),
            in_specs=[any_spec] * 4,
            out_specs=(vmem, vmem, smem),
            scratch_shapes=[
                pltpu.VMEM((per, hidden), BF16),
                pltpu.VMEM((per, hidden), BF16),
                pltpu.SMEM((per,), F32),
                pltpu.VMEM((chans, hidden), BF16),
                pltpu.VMEM((2 * per, hidden), BF16),
                pltpu.VMEM((1, LANES), F32),
                pltpu.VMEM((n, 2 * per, hidden), BF16),
                pltpu.SemaphoreType.DMA((4,)),
                pltpu.SemaphoreType.DMA((2,)),
                pltpu.SemaphoreType.DMA((2,)),
            ],
            compiler_params=pltpu.CompilerParams(collective_id=0, has_side_effects=True),
            name="gather",
        )(mod_scale, mod_shift, step_size, w_in)

        def sweeps(fold, *operands):
            chunks = share * tokens // WIDTH
            return pl.pallas_call(
                functools.partial(sweeps_kernel, n, per, fold),
                out_shape=jax.ShapeDtypeStruct((per, batch, chans, tokens), F32),
                in_specs=[any_spec] + [vmem] * 3 + [smem],
                out_specs=vmem,
                scratch_shapes=[
                    pltpu.VMEM((chunks, chans, WIDTH), F32),
                    pltpu.VMEM((n * per // 2 if fold else 1, hidden, LANES), BF16),
                    pltpu.VMEM((n * per, chans, WIDTH), BF16),
                    pltpu.VMEM((AHEAD, hidden, 2 * WIDTH), F32),
                    pltpu.VMEM((hidden, 2 * WIDTH), BF16),
                    pltpu.VMEM((n * per, chunks, chans, WIDTH), F32),
                    pltpu.SemaphoreType.DMA((chunks,)),
                    pltpu.SemaphoreType.DMA,
                    pltpu.SemaphoreType.DMA,
                ],
                compiler_params=pltpu.CompilerParams(
                    collective_id=1 if fold else 2, has_side_effects=True, vmem_limit_bytes=40 * 1024 * 1024),
                name="sweeps" if fold else "sweeps_wide",
            )(*operands)

        out = lax.cond(
            flag[0] != 0, functools.partial(sweeps, True), functools.partial(sweeps, False),
            jnp.swapaxes(x_init, 1, 2), mods_t, w_in, w_out.T, steps)
        return jnp.swapaxes(out, 2, 3)

    return jax.shard_map(local, mesh=mesh, in_specs=(P("data"), P(), P(), P("time"), P("time"), P("time")), out_specs=P("time", "data"), check_vma=False)
```

```python
import functools
import math

import jax
import jax.numpy as jnp
from jax import lax
from jax.experimental import pallas as pl
from jax.experimental.pallas import tpu as pltpu
from jax.sharding import PartitionSpec as P

SWEEPS = 4
UNROLL = 16
PICKS = 4
EARLY = 9
AHEAD = 2
LANES = 128
WIDTH = 128
FOLD_LIMIT = 2.0 ** 60
C1 = 2.0 * math.sqrt(2.0 / math.pi)
C3 = 8.0 * math.sqrt(2.0 / math.pi) * 0.044715
F32, BF16 = jnp.float32, jnp.bfloat16
MESH = pl.DeviceIdType.MESH
CONTRACT0 = (((0,), (0,)), ((), ()))


def offsets(n):
    return sorted(range(1, n), key=lambda i: (abs(2 * i - n), i))


def signal_all(n, me):
    barrier = pltpu.get_barrier_semaphore()
    for i in offsets(n):
        pl.semaphore_signal(barrier, inc=1, device_id={"time": lax.rem(me + i, n)}, device_id_type=MESH)


def wait_bytes(ref, *sems):
    for sem in sems:
        pltpu.make_async_copy(ref, ref, sem).wait()


def one_hot(cond):
    return jnp.where(cond, 1.0, 0.0).astype(BF16)


def share_parameters(n, me, scale, shift, step, mine, mine_step, mods, steps, send_sem, recv_sem):
    per = scale.shape[0]
    mine[0:per] = scale[...]
    mine[per:2 * per] = shift[...]
    lane = lax.broadcasted_iota(jnp.int32, (1, LANES), 1)
    row = jnp.zeros((1, LANES), F32)
    for i in range(per):
        row = jnp.where(lane == i, step[i], row)
    mine_step[...] = row
    mods[me] = mine[...]
    steps[me] = mine_step[...]
    pl.semaphore_wait(pltpu.get_barrier_semaphore(), n - 1)
    for k, (src, dst) in enumerate(((mine, mods), (mine_step, steps))):
        for i in offsets(n):
            pltpu.make_async_remote_copy(
                src, dst.at[me], send_sem.at[k], recv_sem.at[k],
                device_id={"time": lax.rem(me + i, n)}, device_id_type=MESH).start()


def fold_is_safe(parts, per, w_in):
    top = 0.0
    for part in parts:
        top = jnp.maximum(top, jnp.abs(1.0 + part[:per]))
    return (jnp.max(top) * jnp.max(jnp.abs(w_in.astype(F32))) <= FOLD_LIMIT).astype(jnp.int32)


def scale_row(j, per):
    return j // per * (2 * per) + lax.rem(j, per)


def run_sweeps(n, per, fold, me, get_mods_t, w_in, w_out_t, ready, step_ref, out_ref, x_scr, w_scr, xs_scr, z_scr, h_scr, res_scr, send_sem, recv_sem):
    chunks, chans, width = x_scr.shape
    tokens = res_scr.shape[3]
    cuts = tokens // width
    share = chunks // cuts
    steps = n * per
    tiles = steps // 2
    half_lanes = LANES // 2

    row = lax.broadcasted_iota(jnp.int32, (LANES, LANES), 0)
    lane = lax.broadcasted_iota(jnp.int32, (1, LANES), 1)
    slot = lax.rem(lane, half_lanes)
    spread = one_hot((lax.rem(lane, chans) == row) & (slot < 3 * chans))
    w3 = 0.5 * lax.dot_general(w_in, spread[:chans], CONTRACT0, preferred_element_type=F32)
    wide_row = lax.broadcasted_iota(jnp.int32, (LANES, 2 * LANES), 0)
    wide_lane = lax.broadcasted_iota(jnp.int32, (1, 2 * LANES), 1)

    if fold:
        w3 = w3 + jnp.where(slot == 3 * chans, 0.5, 0.0)
        ones = jnp.where(slot < 3 * chans, 1.0, 0.0)
        rest_lanes = (slot >= chans) & (slot < 3 * chans)
        low_lanes = (slot >= 2 * chans) & (slot < 3 * chans)
        wide_slot = lax.rem(wide_lane, half_lanes)
        source = scale_row(wide_lane // half_lanes, per) + jnp.where(wide_slot == 3 * chans, per, 0)
        source = jnp.where(wide_slot <= 3 * chans, source, -8 * steps)
        ahead = wide_row - source
        mods_t = get_mods_t()

        def build(g, unused):
            picked = []
            for t in range(PICKS):
                first = (g * PICKS + t) * 8
                picked.append(jnp.dot(mods_t, one_hot(ahead == first), preferred_element_type=F32))
            for t in range(PICKS):
                for p in range(2):
                    prod = w3 * (picked[t][:, p * LANES:(p + 1) * LANES] + ones)
                    rest = prod - jnp.where(rest_lanes, prod.astype(BF16).astype(F32), 0.0)
                    rest = rest - jnp.where(low_lanes, rest.astype(BF16).astype(F32), 0.0)
                    w_scr[(g * PICKS + t) * 2 + p] = rest.astype(BF16)
            return unused

        lax.fori_loop(0, steps // (4 * PICKS), build, 0)
    else:
        mods_t = get_mods_t()
        w_scr[0] = (w3 * jnp.where(lane < chans, 2.0, 0.0)).astype(BF16)

    ones_rows = jnp.ones((chans, width), BF16)
    zero_rows = jnp.zeros((half_lanes, width), BF16)
    unroll = UNROLL if fold else 2 * AHEAD
    groups = tiles // unroll
    per_chunk = SWEEPS * groups
    early = max(unroll - EARLY, 0)

    def half_pre(t, x):
        tops = [jnp.concatenate([x[p], x[p], x[p], ones_rows], axis=0) for p in range(2)]
        if fold:
            left = jnp.concatenate([tops[0], zero_rows], axis=0)
            right = jnp.concatenate([zero_rows, tops[1]], axis=0)
            return jnp.dot(w_scr[t], jnp.concatenate([left, right], axis=1), preferred_element_type=F32)
        rhs = jnp.concatenate([jnp.concatenate([top, zero_rows], axis=0) for top in tops], axis=1)
        pre = jnp.dot(w_scr[0], rhs, preferred_element_type=F32)
        src = scale_row(2 * t + wide_lane // width, per)
        scale = jnp.dot(mods_t, one_hot(wide_row == src), preferred_element_type=F32)
        shift = jnp.dot(mods_t, one_hot(wide_row == src + per), preferred_element_type=F32)
        return 0.5 * (pre * (1.0 + scale) + shift)

    def project(hidden):
        return jnp.dot(w_out_t, hidden, preferred_element_type=F32)

    def load_xs(t):
        return xs_scr[2 * t], xs_scr[2 * t + 1]

    def advance(g, t, d, d_prev, total, first=None):
        c = jnp.maximum(g, 0) // per_chunk
        lanes = pl.ds(pl.multiple_of(lax.rem(c, cuts) * width, width), width)
        x0 = x_scr[c]
        x_next = x_scr[jnp.minimum((g + per_chunk) // per_chunk, chunks - 1)]
        last = lax.rem(g + per_chunk, per_chunk) >= per_chunk - groups
        for p in range(2):
            j = 2 * t + p
            i = jnp.maximum(j - 1, 0)
            part = d[:, p * width:(p + 1) * width]
            total = total + step_ref[i // per, 0, lax.rem(i, per)] * (0.5 * (d_prev + part))
            if p == 0 and first is not None:
                total = jnp.where(first, 0.0, total)
            new = x0 + total
            xs_scr[j] = jnp.where(last, x_next, new).astype(BF16)
            res_scr[j, c // cuts, :, lanes] = new
            d_prev = part
        return d_prev, total

    def send(b, cut=None):
        lanes = slice(None) if cut is None else pl.ds(cut * width, width)
        place = (slice(None), me * share + b, slice(None), lanes)
        for i in offsets(n):
            q = lax.rem(me + i, n)
            pltpu.make_async_remote_copy(
                res_scr.at[pl.ds(q * per, per), b, :, lanes], out_ref.at[place], send_sem, recv_sem,
                device_id={"time": q}, device_id_type=MESH).start()
        out_ref[place] = res_scr[pl.ds(me * per, per), b, :, lanes]

    def body(g, carry):
        t0 = lax.rem(g, groups) * unroll
        t_next = lax.rem(g + 1, groups) * unroll
        xs = [load_xs(t0 + u) for u in range(AHEAD, unroll)] + [load_xs(t_next + u) for u in range(AHEAD)]
        ds = [project(h_scr[...])]
        halves = {u: z_scr[u] for u in range(AHEAD)}
        for u in range(unroll):
            v = u + AHEAD
            if v < unroll:
                halves[v] = half_pre(t0 + v, xs[u])
            half = halves.pop(u)
            arg = half * (half * half * C3 + C1)
            hidden = (half * (1.0 + jnp.tanh(arg))).astype(BF16)
            if early <= u < early + AHEAD:
                z_scr[u - early] = half_pre(t_next + u - early, xs[u - early - AHEAD])
            if u < unroll - 1:
                ds.append(project(hidden))
            else:
                h_scr[...] = hidden
        carry = advance(g - 1, lax.rem(t0 + tiles - 1, tiles), ds[0], *carry)
        for u in range(unroll - 1):
            carry = advance(g, t0 + u, ds[u + 1], *carry, first=t0 == 0 if u == 0 else None)

        for c in range(cuts, chunks):
            if c % cuts == 0 or c > chunks - cuts:
                @pl.when(g == c * per_chunk)
                def _(c=c):
                    send((c - 1) // cuts, None if c % cuts == 0 else (c - 1) % cuts)

        return carry

    x_first = x_scr[0].astype(BF16)

    @pl.loop(0, steps)
    def _(j):
        xs_scr[j] = x_first

    for u in range(AHEAD):
        z_scr[u] = half_pre(u, (x_first, x_first))
    h_scr[...] = jnp.zeros_like(h_scr)
    zero = jnp.zeros((chans, width), F32)
    total_groups = chunks * per_chunk
    ready()
    carry = lax.fori_loop(0, total_groups, body, (zero, zero))
    advance(total_groups - 1, tiles - 1, project(h_scr[...]), *carry)
    send(share - 1, cuts - 1)
    wait_bytes(res_scr.at[pl.ds(0, (n - 1) * per)], recv_sem, send_sem)


def x_loads(me, x_hbm, x_scr, sem):
    chunks, _, width = x_scr.shape
    cuts = x_hbm.shape[2] // width
    return [
        pltpu.make_async_copy(
            x_hbm.at[me * (chunks // cuts) + c // cuts, :, pl.ds(c % cuts * width, width)], x_scr.at[c], sem.at[c])
        for c in range(chunks)
    ]


def folded_kernel(n, x_hbm, scale_hbm, shift_hbm, step_hbm, w_in_hbm, w_out_hbm, out_ref, mods_t_ref, steps_ref, flag_ref, scale, shift, step, w_in, w_out_t, mine, mine_step, mods, step_all, load_sem, x_sem, param_send, param_recv, x_scr, w_scr, xs_scr, z_scr, h_scr, res_scr, send_sem, recv_sem):
    me = lax.axis_index("time")
    per = scale.shape[0]
    loads = [
        pltpu.make_async_copy(src, dst, load_sem.at[k])
        for k, (src, dst) in enumerate((
            (scale_hbm, scale), (shift_hbm, shift), (step_hbm, step), (w_in_hbm, w_in), (w_out_hbm, w_out_t)))
    ] + x_loads(me, x_hbm, x_scr, x_sem)
    for load in loads:
        load.start()
    signal_all(n, me)
    for load in loads:
        load.wait()
    share_parameters(n, me, scale, shift, step, mine, mine_step, mods, steps_ref, param_send, param_recv)

    def get_mods_t():
        wait_bytes(mods.at[pl.ds(0, n - 1)], param_recv.at[0])
        parts = [mods[q].astype(F32) for q in range(n)]
        flag_ref[0] = fold_is_safe(parts, per, w_in[...])
        flat = jnp.concatenate(parts, axis=0).astype(BF16)
        r = lax.broadcasted_iota(jnp.int32, (LANES, LANES), 0)
        c = lax.broadcasted_iota(jnp.int32, (LANES, LANES), 1)
        mods_t = lax.dot_general(flat, one_hot(r == c), CONTRACT0, preferred_element_type=F32).astype(BF16)
        mods_t_ref[...] = mods_t
        return mods_t

    def ready():
        wait_bytes(steps_ref.at[pl.ds(0, n - 1)], param_recv.at[1], param_send.at[1])
        wait_bytes(mods.at[pl.ds(0, n - 1)], param_send.at[0])
        to_scalars = pltpu.make_async_copy(steps_ref, step_all, load_sem.at[0])
        to_scalars.start()
        to_scalars.wait()

    run_sweeps(n, per, True, me, get_mods_t, w_in[...], w_out_t[...], ready, step_all, out_ref, x_scr, w_scr, xs_scr, z_scr, h_scr, res_scr, send_sem, recv_sem)


def wide_kernel(n, per, x_hbm, mods_t_ref, w_in_ref, w_out_ref, step_ref, out_ref, x_sem, x_scr, w_scr, xs_scr, z_scr, h_scr, res_scr, send_sem, recv_sem):
    me = lax.axis_index("time")
    loads = x_loads(me, x_hbm, x_scr, x_sem)
    for load in loads:
        load.start()
    signal_all(n, me)
    for load in loads:
        load.wait()

    def ready():
        pl.semaphore_wait(pltpu.get_barrier_semaphore(), n - 1)

    run_sweeps(n, per, False, me, lambda: mods_t_ref[...], w_in_ref[...], w_out_ref[...], ready, step_ref, out_ref, x_scr, w_scr, xs_scr, z_scr, h_scr, res_scr, send_sem, recv_sem)


def solution(mesh):
    n = mesh.shape["time"]
    vmem = pl.BlockSpec(memory_space=pltpu.VMEM)
    smem = pl.BlockSpec(memory_space=pltpu.SMEM)

    def local(x_init, w_in, w_out, mod_scale, mod_shift, step_size):
        batch, tokens, chans = x_init.shape
        per, hidden = mod_scale.shape
        share = batch // n
        any_spec = pl.BlockSpec(memory_space=pl.ANY)
        steps = n * per
        chunks = share * tokens // WIDTH
        x_t = jnp.swapaxes(x_init, 1, 2)
        out_type = jax.ShapeDtypeStruct((per, batch, chans, tokens), F32)
        dma = pltpu.SemaphoreType.DMA

        def scratch(folded):
            return [
                pltpu.VMEM((chunks, chans, WIDTH), F32),
                pltpu.VMEM((steps // 2 if folded else 1, hidden, LANES), BF16),
                pltpu.VMEM((steps, chans, WIDTH), BF16),
                pltpu.VMEM((AHEAD, hidden, 2 * WIDTH), F32),
                pltpu.VMEM((hidden, 2 * WIDTH), BF16),
                pltpu.VMEM((steps, share, chans, tokens), F32),
                dma,
                dma,
            ]

        out, mods_t, step_all, flag = pl.pallas_call(
            functools.partial(folded_kernel, n),
            out_shape=(
                out_type,
                jax.ShapeDtypeStruct((hidden, LANES), BF16),
                jax.ShapeDtypeStruct((n, 1, LANES), F32),
                jax.ShapeDtypeStruct((1,), jnp.int32),
            ),
            in_specs=[any_spec] * 6,
            out_specs=(vmem, vmem, vmem, smem),
            scratch_shapes=[
                pltpu.VMEM((per, hidden), BF16),
                pltpu.VMEM((per, hidden), BF16),
                pltpu.SMEM((per,), F32),
                pltpu.VMEM((chans, hidden), BF16),
                pltpu.VMEM((chans, hidden), BF16),
                pltpu.VMEM((2 * per, hidden), BF16),
                pltpu.VMEM((1, LANES), F32),
                pltpu.VMEM((n, 2 * per, hidden), BF16),
                pltpu.SMEM((n, 1, LANES), F32),
                dma((5,)),
                dma((chunks,)),
                dma((2,)),
                dma((2,)),
            ] + scratch(True),
            compiler_params=pltpu.CompilerParams(collective_id=0, has_side_effects=True, vmem_limit_bytes=56 * 1024 * 1024),
            name="folded",
        )(x_t, mod_scale, mod_shift, step_size, w_in, w_out.T)

        def wide(out, mods_t, step_all):
            return pl.pallas_call(
                functools.partial(wide_kernel, n, per),
                out_shape=out_type,
                in_specs=[any_spec] + [vmem] * 3 + [smem],
                out_specs=vmem,
                scratch_shapes=[dma((chunks,))] + scratch(False),
                compiler_params=pltpu.CompilerParams(collective_id=1, has_side_effects=True, vmem_limit_bytes=40 * 1024 * 1024),
                name="wide",
            )(x_t, mods_t, w_in, w_out.T, step_all)

        out = lax.cond(flag[0] != 0, lambda out, *rest: out, wide, out, mods_t, step_all)
        return jnp.swapaxes(out, 2, 3)

    return jax.shard_map(local, mesh=mesh, in_specs=(P("data"), P(), P(), P("time"), P("time"), P("time")), out_specs=P("time", "data"), check_vma=False)
```

```python
import functools
import math

import jax
import jax.numpy as jnp
from jax import lax
from jax.experimental import pallas as pl
from jax.experimental.pallas import tpu as pltpu
from jax.sharding import PartitionSpec as P

SWEEPS = 4
UNROLL = 16
PICKS = 4
EARLY = 9
AHEAD = 2
LANES = 128
WIDTH = 128
FOLD_LIMIT = 2.0 ** 60
C1 = 2.0 * math.sqrt(2.0 / math.pi)
C3 = 8.0 * math.sqrt(2.0 / math.pi) * 0.044715
F32, BF16 = jnp.float32, jnp.bfloat16
MESH = pl.DeviceIdType.MESH
CONTRACT0 = (((0,), (0,)), ((), ()))


def offsets(n):
    return sorted(range(1, n), key=lambda i: (abs(2 * i - n), i))


def signal_all(n, me):
    barrier = pltpu.get_barrier_semaphore()
    for i in offsets(n):
        pl.semaphore_signal(barrier, inc=1, device_id={"time": lax.rem(me + i, n)}, device_id_type=MESH)


def wait_bytes(ref, *sems):
    for sem in sems:
        pltpu.make_async_copy(ref, ref, sem).wait()


def one_hot(cond):
    return jnp.where(cond, 1.0, 0.0).astype(BF16)


def share_parameters(n, me, scale, shift, step, mine, mine_step, mods, steps, send_sem, recv_sem):
    per = scale.shape[0]
    mine[0:per] = scale[...]
    mine[per:2 * per] = shift[...]
    lane = lax.broadcasted_iota(jnp.int32, (1, LANES), 1)
    row = jnp.zeros((1, LANES), F32)
    for i in range(per):
        row = jnp.where(lane == i, step[i], row)
    mine_step[...] = row
    mods[me] = mine[...]
    steps[me] = mine_step[...]
    pl.semaphore_wait(pltpu.get_barrier_semaphore(), n - 1)
    for k, (src, dst) in enumerate(((mine, mods), (mine_step, steps))):
        for i in offsets(n):
            pltpu.make_async_remote_copy(
                src, dst.at[me], send_sem.at[k], recv_sem.at[k],
                device_id={"time": lax.rem(me + i, n)}, device_id_type=MESH).start()


def fold_is_safe(parts, per, w_in):
    top = 0.0
    for part in parts:
        top = jnp.maximum(top, jnp.abs(1.0 + part[:per]))
    return (jnp.max(top) * jnp.max(jnp.abs(w_in.astype(F32))) <= FOLD_LIMIT).astype(jnp.int32)


def scale_row(j, per):
    return j // per * (2 * per) + lax.rem(j, per)


def run_sweeps(n, per, fold, me, get_mods_t, w_in, w_out_t, ready, step_ref, out_ref, x_scr, w_scr, xs_scr, z_scr, h_scr, res_scr, send_sem, recv_sem):
    chunks, chans, width = x_scr.shape
    tokens = res_scr.shape[3]
    cuts = tokens // width
    share = chunks // cuts
    steps = n * per
    tiles = steps // 2
    half_lanes = LANES // 2

    row = lax.broadcasted_iota(jnp.int32, (LANES, LANES), 0)
    lane = lax.broadcasted_iota(jnp.int32, (1, LANES), 1)
    slot = lax.rem(lane, half_lanes)
    spread = one_hot((lax.rem(lane, chans) == row) & (slot < 3 * chans))
    w3 = 0.5 * lax.dot_general(w_in, spread[:chans], CONTRACT0, preferred_element_type=F32)
    wide_row = lax.broadcasted_iota(jnp.int32, (LANES, 2 * LANES), 0)
    wide_lane = lax.broadcasted_iota(jnp.int32, (1, 2 * LANES), 1)

    if fold:
        fixed = jnp.where(slot < chans, w3, 0.0)
        w3 = w3 + jnp.where(slot == 3 * chans, 0.5, 0.0)
        low_lanes = (slot >= 2 * chans) & (slot < 3 * chans)
        wide_slot = lax.rem(wide_lane, half_lanes)
        source = scale_row(wide_lane // half_lanes, per) + jnp.where(wide_slot == 3 * chans, per, 0)
        source = jnp.where((wide_slot >= chans) & (wide_slot <= 3 * chans), source, -8 * steps)
        ahead = wide_row - source
        mods_t = get_mods_t()

        def build(g, unused):
            picked = []
            for t in range(PICKS):
                first = (g * PICKS + t) * 8
                picked.append(jnp.dot(mods_t, one_hot(ahead == first), preferred_element_type=F32))
            for t in range(PICKS):
                for p in range(2):
                    prod = w3 * picked[t][:, p * LANES:(p + 1) * LANES] + fixed
                    rest = prod - jnp.where(low_lanes, prod.astype(BF16).astype(F32), 0.0)
                    w_scr[(g * PICKS + t) * 2 + p] = rest.astype(BF16)
            return unused

        lax.fori_loop(0, steps // (4 * PICKS), build, 0)
    else:
        mods_t = get_mods_t()
        w_scr[0] = (w3 * jnp.where(lane < chans, 2.0, 0.0)).astype(BF16)

    ones_rows = jnp.ones((chans, width), BF16)
    zero_rows = jnp.zeros((half_lanes, width), BF16)
    unroll = UNROLL if fold else 2 * AHEAD
    groups = tiles // unroll
    per_chunk = SWEEPS * groups
    early = max(unroll - EARLY, 0)

    def half_pre(t, x):
        tops = [jnp.concatenate([x[p], x[p], x[p], ones_rows], axis=0) for p in range(2)]
        if fold:
            left = jnp.concatenate([tops[0], zero_rows], axis=0)
            right = jnp.concatenate([zero_rows, tops[1]], axis=0)
            return jnp.dot(w_scr[t], jnp.concatenate([left, right], axis=1), preferred_element_type=F32)
        rhs = jnp.concatenate([jnp.concatenate([top, zero_rows], axis=0) for top in tops], axis=1)
        pre = jnp.dot(w_scr[0], rhs, preferred_element_type=F32)
        src = scale_row(2 * t + wide_lane // width, per)
        scale = jnp.dot(mods_t, one_hot(wide_row == src), preferred_element_type=F32)
        shift = jnp.dot(mods_t, one_hot(wide_row == src + per), preferred_element_type=F32)
        return 0.5 * (pre * (1.0 + scale) + shift)

    def project(hidden):
        return jnp.dot(w_out_t, hidden, preferred_element_type=F32)

    def load_xs(t):
        return xs_scr[2 * t], xs_scr[2 * t + 1]

    def advance(g, t, d, d_prev, total, first=None):
        c = jnp.maximum(g, 0) // per_chunk
        lanes = pl.ds(pl.multiple_of(lax.rem(c, cuts) * width, width), width)
        x0 = x_scr[c]
        x_next = x_scr[jnp.minimum((g + per_chunk) // per_chunk, chunks - 1)]
        last = lax.rem(g + per_chunk, per_chunk) >= per_chunk - groups
        for p in range(2):
            j = 2 * t + p
            i = jnp.maximum(j - 1, 0)
            part = d[:, p * width:(p + 1) * width]
            total = total + (0.5 * step_ref[i // per, 0, lax.rem(i, per)]) * (d_prev + part)
            if p == 0 and first is not None:
                total = jnp.where(first, 0.0, total)
            new = x0 + total
            xs_scr[j] = jnp.where(last, x_next, new).astype(BF16)
            res_scr[j, c // cuts, :, lanes] = new
            d_prev = part
        return d_prev, total

    def send(b, cut=None):
        lanes = slice(None) if cut is None else pl.ds(cut * width, width)
        place = (slice(None), me * share + b, slice(None), lanes)
        for i in offsets(n):
            q = lax.rem(me + i, n)
            pltpu.make_async_remote_copy(
                res_scr.at[pl.ds(q * per, per), b, :, lanes], out_ref.at[place], send_sem, recv_sem,
                device_id={"time": q}, device_id_type=MESH).start()
        out_ref[place] = res_scr[pl.ds(me * per, per), b, :, lanes]

    def body(g, carry):
        t0 = lax.rem(g, groups) * unroll
        t_next = lax.rem(g + 1, groups) * unroll
        xs = [load_xs(t0 + u) for u in range(AHEAD, unroll)] + [load_xs(t_next + u) for u in range(AHEAD)]
        ds = [project(h_scr[...])]
        halves = {u: z_scr[u] for u in range(AHEAD)}
        for u in range(unroll):
            v = u + AHEAD
            if v < unroll:
                halves[v] = half_pre(t0 + v, xs[u])
            half = halves.pop(u)
            arg = half * (half * half * C3 + C1)
            hidden = (half * (1.0 + jnp.tanh(arg))).astype(BF16)
            if early <= u < early + AHEAD:
                z_scr[u - early] = half_pre(t_next + u - early, xs[u - early - AHEAD])
            if u < unroll - 1:
                ds.append(project(hidden))
            else:
                h_scr[...] = hidden
        carry = advance(g - 1, lax.rem(t0 + tiles - 1, tiles), ds[0], *carry)
        for u in range(unroll - 1):
            carry = advance(g, t0 + u, ds[u + 1], *carry, first=t0 == 0 if u == 0 else None)

        for c in range(cuts, chunks):
            if c % cuts == 0 or c > chunks - cuts:
                @pl.when(g == c * per_chunk)
                def _(c=c):
                    send((c - 1) // cuts, None if c % cuts == 0 else (c - 1) % cuts)

        return carry

    x_first = x_scr[0].astype(BF16)

    @pl.loop(0, steps)
    def _(j):
        xs_scr[j] = x_first

    for u in range(AHEAD):
        z_scr[u] = half_pre(u, (x_first, x_first))
    h_scr[...] = jnp.zeros_like(h_scr)
    zero = jnp.zeros((chans, width), F32)
    total_groups = chunks * per_chunk
    ready()
    carry = lax.fori_loop(0, total_groups, body, (zero, zero))
    advance(total_groups - 1, tiles - 1, project(h_scr[...]), *carry)
    send(share - 1, cuts - 1)
    wait_bytes(res_scr.at[pl.ds(0, (n - 1) * per)], recv_sem, send_sem)


def x_loads(me, x_hbm, x_scr, sem):
    chunks, _, width = x_scr.shape
    cuts = x_hbm.shape[2] // width
    return [
        pltpu.make_async_copy(
            x_hbm.at[me * (chunks // cuts) + c // cuts, :, pl.ds(c % cuts * width, width)], x_scr.at[c], sem.at[c])
        for c in range(chunks)
    ]


def folded_kernel(n, x_hbm, scale_hbm, shift_hbm, step_hbm, w_in_hbm, w_out_hbm, out_ref, mods_t_ref, steps_ref, flag_ref, scale, shift, step, w_in, w_out_t, mine, mine_step, mods, step_all, load_sem, x_sem, param_send, param_recv, x_scr, w_scr, xs_scr, z_scr, h_scr, res_scr, send_sem, recv_sem):
    me = lax.axis_index("time")
    per = scale.shape[0]
    loads = [
        pltpu.make_async_copy(src, dst, load_sem.at[k])
        for k, (src, dst) in enumerate((
            (scale_hbm, scale), (shift_hbm, shift), (step_hbm, step), (w_in_hbm, w_in), (w_out_hbm, w_out_t)))
    ] + x_loads(me, x_hbm, x_scr, x_sem)
    for load in loads:
        load.start()
    signal_all(n, me)
    for load in loads:
        load.wait()
    share_parameters(n, me, scale, shift, step, mine, mine_step, mods, steps_ref, param_send, param_recv)

    def get_mods_t():
        wait_bytes(mods.at[pl.ds(0, n - 1)], param_recv.at[0])
        parts = [mods[q].astype(F32) for q in range(n)]
        flag_ref[0] = fold_is_safe(parts, per, w_in[...])
        flat = jnp.concatenate(parts, axis=0).astype(BF16)
        r = lax.broadcasted_iota(jnp.int32, (LANES, LANES), 0)
        c = lax.broadcasted_iota(jnp.int32, (LANES, LANES), 1)
        mods_t = lax.dot_general(flat, one_hot(r == c), CONTRACT0, preferred_element_type=F32).astype(BF16)
        mods_t_ref[...] = mods_t
        return mods_t

    def ready():
        wait_bytes(steps_ref.at[pl.ds(0, n - 1)], param_recv.at[1], param_send.at[1])
        wait_bytes(mods.at[pl.ds(0, n - 1)], param_send.at[0])
        to_scalars = pltpu.make_async_copy(steps_ref, step_all, load_sem.at[0])
        to_scalars.start()
        to_scalars.wait()

    run_sweeps(n, per, True, me, get_mods_t, w_in[...], w_out_t[...], ready, step_all, out_ref, x_scr, w_scr, xs_scr, z_scr, h_scr, res_scr, send_sem, recv_sem)


def wide_kernel(n, per, x_hbm, mods_t_ref, w_in_ref, w_out_ref, step_ref, out_ref, x_sem, x_scr, w_scr, xs_scr, z_scr, h_scr, res_scr, send_sem, recv_sem):
    me = lax.axis_index("time")
    loads = x_loads(me, x_hbm, x_scr, x_sem)
    for load in loads:
        load.start()
    signal_all(n, me)
    for load in loads:
        load.wait()

    def ready():
        pl.semaphore_wait(pltpu.get_barrier_semaphore(), n - 1)

    run_sweeps(n, per, False, me, lambda: mods_t_ref[...], w_in_ref[...], w_out_ref[...], ready, step_ref, out_ref, x_scr, w_scr, xs_scr, z_scr, h_scr, res_scr, send_sem, recv_sem)


def solution(mesh):
    n = mesh.shape["time"]
    vmem = pl.BlockSpec(memory_space=pltpu.VMEM)
    smem = pl.BlockSpec(memory_space=pltpu.SMEM)

    def local(x_init, w_in, w_out, mod_scale, mod_shift, step_size):
        batch, tokens, chans = x_init.shape
        per, hidden = mod_scale.shape
        share = batch // n
        any_spec = pl.BlockSpec(memory_space=pl.ANY)
        steps = n * per
        chunks = share * tokens // WIDTH
        x_t = jnp.swapaxes(x_init, 1, 2)
        out_type = jax.ShapeDtypeStruct((per, batch, chans, tokens), F32)
        dma = pltpu.SemaphoreType.DMA

        def scratch(folded):
            return [
                pltpu.VMEM((chunks, chans, WIDTH), F32),
                pltpu.VMEM((steps // 2 if folded else 1, hidden, LANES), BF16),
                pltpu.VMEM((steps, chans, WIDTH), BF16),
                pltpu.VMEM((AHEAD, hidden, 2 * WIDTH), F32),
                pltpu.VMEM((hidden, 2 * WIDTH), BF16),
                pltpu.VMEM((steps, share, chans, tokens), F32),
                dma,
                dma,
            ]

        out, mods_t, step_all, flag = pl.pallas_call(
            functools.partial(folded_kernel, n),
            out_shape=(
                out_type,
                jax.ShapeDtypeStruct((hidden, LANES), BF16),
                jax.ShapeDtypeStruct((n, 1, LANES), F32),
                jax.ShapeDtypeStruct((1,), jnp.int32),
            ),
            in_specs=[any_spec] * 6,
            out_specs=(vmem, vmem, vmem, smem),
            scratch_shapes=[
                pltpu.VMEM((per, hidden), BF16),
                pltpu.VMEM((per, hidden), BF16),
                pltpu.SMEM((per,), F32),
                pltpu.VMEM((chans, hidden), BF16),
                pltpu.VMEM((chans, hidden), BF16),
                pltpu.VMEM((2 * per, hidden), BF16),
                pltpu.VMEM((1, LANES), F32),
                pltpu.VMEM((n, 2 * per, hidden), BF16),
                pltpu.SMEM((n, 1, LANES), F32),
                dma((5,)),
                dma((chunks,)),
                dma((2,)),
                dma((2,)),
            ] + scratch(True),
            compiler_params=pltpu.CompilerParams(collective_id=0, has_side_effects=True, vmem_limit_bytes=56 * 1024 * 1024),
            name="folded",
        )(x_t, mod_scale, mod_shift, step_size, w_in, w_out.T)

        def wide(out, mods_t, step_all):
            return pl.pallas_call(
                functools.partial(wide_kernel, n, per),
                out_shape=out_type,
                in_specs=[any_spec] + [vmem] * 3 + [smem],
                out_specs=vmem,
                scratch_shapes=[dma((chunks,))] + scratch(False),
                compiler_params=pltpu.CompilerParams(collective_id=1, has_side_effects=True, vmem_limit_bytes=40 * 1024 * 1024),
                name="wide",
            )(x_t, mods_t, w_in, w_out.T, step_all)

        out = lax.cond(flag[0] != 0, lambda out, *rest: out, wide, out, mods_t, step_all)
        return jnp.swapaxes(out, 2, 3)

    return jax.shard_map(local, mesh=mesh, in_specs=(P("data"), P(), P(), P("time"), P("time"), P("time")), out_specs=P("time", "data"), check_vma=False)
```

```python
import functools
import math

import jax
import jax.numpy as jnp
from jax import lax
from jax.experimental import pallas as pl
from jax.experimental.pallas import tpu as pltpu
from jax.sharding import PartitionSpec as P

SWEEPS = 4
UNROLL = 16
GROUPS = 4
EARLY = 9
AHEAD = 2
LANES = 128
WIDTH = 128
FOLD_LIMIT = 2.0 ** 60
C1 = 2.0 * math.sqrt(2.0 / math.pi)
C3 = 8.0 * math.sqrt(2.0 / math.pi) * 0.044715
F32, BF16 = jnp.float32, jnp.bfloat16
MESH = pl.DeviceIdType.MESH
CONTRACT0 = (((0,), (0,)), ((), ()))


def offsets(n):
    return sorted(range(1, n), key=lambda i: (abs(2 * i - n), i))


def signal_all(n, me):
    barrier = pltpu.get_barrier_semaphore()
    for i in offsets(n):
        pl.semaphore_signal(barrier, inc=1, device_id={"time": lax.rem(me + i, n)}, device_id_type=MESH)


def wait_bytes(ref, *sems):
    for sem in sems:
        pltpu.make_async_copy(ref, ref, sem).wait()


def one_hot(cond):
    return jnp.where(cond, 1.0, 0.0).astype(BF16)


def share_parameters(n, me, scale, shift, step, mine, mine_step, mods, steps, send_sem, recv_sem):
    per = scale.shape[0]
    mine[0:per] = scale[...]
    mine[per:2 * per] = shift[...]
    lane = lax.broadcasted_iota(jnp.int32, (1, LANES), 1)
    row = jnp.zeros((1, LANES), F32)
    for i in range(per):
        row = jnp.where(lane == i, step[i], row)
    mine_step[...] = row
    mods[me] = mine[...]
    steps[me] = mine_step[...]
    pl.semaphore_wait(pltpu.get_barrier_semaphore(), n - 1)
    size = n // GROUPS
    for i in offsets(n):
        q = lax.rem(me + i, n)
        group = lax.rem(me // size - q // size + GROUPS, GROUPS)
        pltpu.make_async_remote_copy(
            mine, mods.at[me], send_sem.at[0], recv_sem.at[group], device_id={"time": q}, device_id_type=MESH).start()
    for i in offsets(n):
        pltpu.make_async_remote_copy(
            mine_step, steps.at[me], send_sem.at[1], recv_sem.at[GROUPS],
            device_id={"time": lax.rem(me + i, n)}, device_id_type=MESH).start()


def transposed(parts):
    rows = jnp.concatenate(parts, axis=0)
    if rows.shape[0] < LANES:
        rows = jnp.concatenate([rows, jnp.zeros((LANES - rows.shape[0], rows.shape[1]), F32)], axis=0)
    return rows.T.astype(BF16)


def scale_row(j, per):
    return j // per * (2 * per) + lax.rem(j, per)


def run_sweeps(n, per, fold, me, get_mods, w_in, w_out_t, ready, step_ref, out_ref, x_scr, w_scr, xs_scr, z_scr, h_scr, res_scr, send_sem, recv_sem):
    chunks, chans, width = x_scr.shape
    tokens = res_scr.shape[3]
    cuts = tokens // width
    share = chunks // cuts
    steps = n * per
    tiles = steps // 2
    half_lanes = LANES // 2

    row = lax.broadcasted_iota(jnp.int32, (LANES, LANES), 0)
    x_first = x_scr[0].astype(BF16)

    @pl.loop(0, steps)
    def _(j):
        xs_scr[j] = x_first

    h_scr[...] = jnp.zeros_like(h_scr)
    lane = lax.broadcasted_iota(jnp.int32, (1, LANES), 1)
    slot = lax.rem(lane, half_lanes)
    spread = one_hot((lax.rem(lane, chans) == row) & (slot < 3 * chans))
    w3 = 0.5 * lax.dot_general(w_in, spread[:chans], CONTRACT0, preferred_element_type=F32)
    wide_row = lax.broadcasted_iota(jnp.int32, (LANES, 2 * LANES), 0)
    wide_lane = lax.broadcasted_iota(jnp.int32, (1, 2 * LANES), 1)

    if fold:
        fixed = jnp.where(slot < chans, w3, 0.0)
        w3 = w3 + jnp.where(slot == 3 * chans, 0.5, 0.0)
        low_lanes = (slot >= 2 * chans) & (slot < 3 * chans)
        wide_slot = lax.rem(wide_lane, half_lanes)
        source = scale_row(wide_lane // half_lanes, per) + jnp.where(wide_slot == 3 * chans, per, 0)
        source = jnp.where((wide_slot >= chans) & (wide_slot <= 3 * chans), source, -8 * steps)
        picks = [one_hot(wide_row - 8 * t == source) for t in range(n // GROUPS * per // 4)]
        for k in range(GROUPS):
            first, mods_t = get_mods(k)
            picked = [jnp.dot(mods_t, pick, preferred_element_type=F32) for pick in picks]
            for t in range(2 * len(picks)):
                mod = picked[t // 2][:, t % 2 * LANES:(t % 2 + 1) * LANES]
                prod = w3 * mod + fixed
                rest = prod - jnp.where(low_lanes, prod.astype(BF16).astype(F32), 0.0)
                w_scr[first * per // 2 + t] = rest.astype(BF16)
    else:
        mods_t = get_mods()
        w_scr[0] = (w3 * jnp.where(lane < chans, 2.0, 0.0)).astype(BF16)

    ones_rows = jnp.ones((chans, width), BF16)
    zero_rows = jnp.zeros((half_lanes, width), BF16)
    unroll = UNROLL if fold else 2 * AHEAD
    groups = tiles // unroll
    per_chunk = SWEEPS * groups
    early = max(unroll - EARLY, 0)

    def half_pre(t, x):
        tops = [jnp.concatenate([x[p], x[p], x[p], ones_rows], axis=0) for p in range(2)]
        if fold:
            left = jnp.concatenate([tops[0], zero_rows], axis=0)
            right = jnp.concatenate([zero_rows, tops[1]], axis=0)
            return jnp.dot(w_scr[t], jnp.concatenate([left, right], axis=1), preferred_element_type=F32)
        rhs = jnp.concatenate([jnp.concatenate([top, zero_rows], axis=0) for top in tops], axis=1)
        pre = jnp.dot(w_scr[0], rhs, preferred_element_type=F32)
        src = scale_row(2 * t + wide_lane // width, per)
        scale = jnp.dot(mods_t, one_hot(wide_row == src), preferred_element_type=F32)
        shift = jnp.dot(mods_t, one_hot(wide_row == src + per), preferred_element_type=F32)
        return 0.5 * (pre * (1.0 + scale) + shift)

    def project(hidden):
        return jnp.dot(w_out_t, hidden, preferred_element_type=F32)

    def load_xs(t):
        return xs_scr[2 * t], xs_scr[2 * t + 1]

    def advance(g, t, d, d_prev, total, first=None):
        c = jnp.maximum(g, 0) // per_chunk
        lanes = pl.ds(pl.multiple_of(lax.rem(c, cuts) * width, width), width)
        x0 = x_scr[c]
        x_next = x_scr[jnp.minimum((g + per_chunk) // per_chunk, chunks - 1)]
        last = lax.rem(g + per_chunk, per_chunk) >= per_chunk - groups
        for p in range(2):
            j = 2 * t + p
            i = jnp.maximum(j - 1, 0)
            part = d[:, p * width:(p + 1) * width]
            total = total + (0.5 * step_ref[i // per, 0, lax.rem(i, per)]) * (d_prev + part)
            if p == 0 and first is not None:
                total = jnp.where(first, 0.0, total)
            new = x0 + total
            xs_scr[j] = jnp.where(last, x_next, new).astype(BF16)
            res_scr[j, c // cuts, :, lanes] = new
            d_prev = part
        return d_prev, total

    def send(b, cut=None):
        lanes = slice(None) if cut is None else pl.ds(cut * width, width)
        place = (slice(None), me * share + b, slice(None), lanes)
        for i in offsets(n):
            q = lax.rem(me + i, n)
            pltpu.make_async_remote_copy(
                res_scr.at[pl.ds(q * per, per), b, :, lanes], out_ref.at[place], send_sem, recv_sem,
                device_id={"time": q}, device_id_type=MESH).start()
        out_ref[place] = res_scr[pl.ds(me * per, per), b, :, lanes]

    def body(g, carry):
        t0 = lax.rem(g, groups) * unroll
        t_next = lax.rem(g + 1, groups) * unroll
        xs = [load_xs(t0 + u) for u in range(AHEAD, unroll)] + [load_xs(t_next + u) for u in range(AHEAD)]
        ds = [project(h_scr[...])]
        halves = {u: z_scr[u] for u in range(AHEAD)}
        for u in range(unroll):
            v = u + AHEAD
            if v < unroll:
                halves[v] = half_pre(t0 + v, xs[u])
            half = halves.pop(u)
            arg = half * (half * half * C3 + C1)
            hidden = (half * (1.0 + jnp.tanh(arg))).astype(BF16)
            if early <= u < early + AHEAD:
                z_scr[u - early] = half_pre(t_next + u - early, xs[u - early - AHEAD])
            if u < unroll - 1:
                ds.append(project(hidden))
            else:
                h_scr[...] = hidden
        carry = advance(g - 1, lax.rem(t0 + tiles - 1, tiles), ds[0], *carry)
        for u in range(unroll - 1):
            carry = advance(g, t0 + u, ds[u + 1], *carry, first=t0 == 0 if u == 0 else None)

        for c in range(cuts, chunks):
            if c % cuts == 0 or c > chunks - cuts:
                @pl.when(g == c * per_chunk)
                def _(c=c):
                    send((c - 1) // cuts, None if c % cuts == 0 else (c - 1) % cuts)

        return carry

    for u in range(AHEAD):
        z_scr[u] = half_pre(u, (x_first, x_first))
    zero = jnp.zeros((chans, width), F32)
    total_groups = chunks * per_chunk
    ready()
    carry = lax.fori_loop(0, total_groups, body, (zero, zero))
    advance(total_groups - 1, tiles - 1, project(h_scr[...]), *carry)
    send(share - 1, cuts - 1)
    wait_bytes(res_scr.at[pl.ds(0, (n - 1) * per)], recv_sem, send_sem)


def x_loads(me, x_hbm, x_scr, sem):
    chunks, _, width = x_scr.shape
    cuts = x_hbm.shape[2] // width
    return [
        pltpu.make_async_copy(
            x_hbm.at[me * (chunks // cuts) + c // cuts, :, pl.ds(c % cuts * width, width)], x_scr.at[c], sem.at[c])
        for c in range(chunks)
    ]


def folded_kernel(n, x_hbm, scale_hbm, shift_hbm, step_hbm, w_in_hbm, w_out_hbm, out_ref, mods, steps_ref, flag_ref, scale, shift, step, w_in, w_out_t, mine, mine_step, step_all, load_sem, x_sem, param_send, param_recv, x_scr, w_scr, xs_scr, z_scr, h_scr, res_scr, send_sem, recv_sem):
    me = lax.axis_index("time")
    per = scale.shape[0]
    loads = [
        pltpu.make_async_copy(src, dst, load_sem.at[k])
        for k, (src, dst) in enumerate((
            (scale_hbm, scale), (shift_hbm, shift), (step_hbm, step), (w_in_hbm, w_in), (w_out_hbm, w_out_t)))
    ] + x_loads(me, x_hbm, x_scr, x_sem)
    for load in loads:
        load.start()
    signal_all(n, me)
    for load in loads:
        load.wait()
    share_parameters(n, me, scale, shift, step, mine, mine_step, mods, steps_ref, param_send, param_recv)

    tops = []

    def get_mods(k):
        size = n // GROUPS
        wait_bytes(mods.at[pl.ds(0, size if k else size - 1)], param_recv.at[k])
        first = lax.rem(me // size + k, GROUPS) * size
        parts = [mods[first + q].astype(F32) for q in range(size)]
        tops.extend(jnp.abs(1.0 + part[:per]) for part in parts)
        return first, transposed(parts)

    def ready():
        top = functools.reduce(jnp.maximum, tops)
        flag_ref[0] = (jnp.max(top) * jnp.max(jnp.abs(w_in[...].astype(F32))) <= FOLD_LIMIT).astype(jnp.int32)
        wait_bytes(steps_ref.at[pl.ds(0, n - 1)], param_recv.at[GROUPS], param_send.at[1])
        wait_bytes(mods.at[pl.ds(0, n - 1)], param_send.at[0])
        to_scalars = pltpu.make_async_copy(steps_ref, step_all, load_sem.at[0])
        to_scalars.start()
        to_scalars.wait()

    run_sweeps(n, per, True, me, get_mods, w_in[...], w_out_t[...], ready, step_all, out_ref, x_scr, w_scr, xs_scr, z_scr, h_scr, res_scr, send_sem, recv_sem)


def wide_kernel(n, per, x_hbm, mods, w_in_ref, w_out_ref, step_ref, out_ref, x_sem, x_scr, w_scr, xs_scr, z_scr, h_scr, res_scr, send_sem, recv_sem):
    me = lax.axis_index("time")
    loads = x_loads(me, x_hbm, x_scr, x_sem)
    for load in loads:
        load.start()
    signal_all(n, me)
    for load in loads:
        load.wait()

    def ready():
        pl.semaphore_wait(pltpu.get_barrier_semaphore(), n - 1)

    run_sweeps(n, per, False, me, lambda: transposed([mods[q].astype(F32) for q in range(n)]), w_in_ref[...], w_out_ref[...], ready, step_ref, out_ref, x_scr, w_scr, xs_scr, z_scr, h_scr, res_scr, send_sem, recv_sem)


def solution(mesh):
    n = mesh.shape["time"]
    vmem = pl.BlockSpec(memory_space=pltpu.VMEM)
    smem = pl.BlockSpec(memory_space=pltpu.SMEM)

    def local(x_init, w_in, w_out, mod_scale, mod_shift, step_size):
        batch, tokens, chans = x_init.shape
        per, hidden = mod_scale.shape
        share = batch // n
        any_spec = pl.BlockSpec(memory_space=pl.ANY)
        steps = n * per
        chunks = share * tokens // WIDTH
        x_t = jnp.swapaxes(x_init, 1, 2)
        out_type = jax.ShapeDtypeStruct((per, batch, chans, tokens), F32)
        dma = pltpu.SemaphoreType.DMA

        def scratch(folded):
            return [
                pltpu.VMEM((chunks, chans, WIDTH), F32),
                pltpu.VMEM((steps // 2 if folded else 1, hidden, LANES), BF16),
                pltpu.VMEM((steps, chans, WIDTH), BF16),
                pltpu.VMEM((AHEAD, hidden, 2 * WIDTH), F32),
                pltpu.VMEM((hidden, 2 * WIDTH), BF16),
                pltpu.VMEM((steps, share, chans, tokens), F32),
                dma,
                dma,
            ]

        out, mods, step_all, flag = pl.pallas_call(
            functools.partial(folded_kernel, n),
            out_shape=(
                out_type,
                jax.ShapeDtypeStruct((n, 2 * per, hidden), BF16),
                jax.ShapeDtypeStruct((n, 1, LANES), F32),
                jax.ShapeDtypeStruct((1,), jnp.int32),
            ),
            in_specs=[any_spec] * 6,
            out_specs=(vmem, vmem, vmem, smem),
            scratch_shapes=[
                pltpu.VMEM((per, hidden), BF16),
                pltpu.VMEM((per, hidden), BF16),
                pltpu.SMEM((per,), F32),
                pltpu.VMEM((chans, hidden), BF16),
                pltpu.VMEM((chans, hidden), BF16),
                pltpu.VMEM((2 * per, hidden), BF16),
                pltpu.VMEM((1, LANES), F32),
                pltpu.SMEM((n, 1, LANES), F32),
                dma((5,)),
                dma((chunks,)),
                dma((2,)),
                dma((GROUPS + 1,)),
            ] + scratch(True),
            compiler_params=pltpu.CompilerParams(collective_id=0, has_side_effects=True, vmem_limit_bytes=56 * 1024 * 1024),
            name="folded",
        )(x_t, mod_scale, mod_shift, step_size, w_in, w_out.T)

        def wide(out, mods, step_all):
            return pl.pallas_call(
                functools.partial(wide_kernel, n, per),
                out_shape=out_type,
                in_specs=[any_spec] + [vmem] * 3 + [smem],
                out_specs=vmem,
                scratch_shapes=[dma((chunks,))] + scratch(False),
                compiler_params=pltpu.CompilerParams(collective_id=1, has_side_effects=True, vmem_limit_bytes=40 * 1024 * 1024),
                name="wide",
            )(x_t, mods, w_in, w_out.T, step_all)

        out = lax.cond(flag[0] != 0, lambda out, *rest: out, wide, out, mods, step_all)
        return jnp.swapaxes(out, 2, 3)

    return jax.shard_map(local, mesh=mesh, in_specs=(P("data"), P(), P(), P("time"), P("time"), P("time")), out_specs=P("time", "data"), check_vma=False)
```

```python
import functools
import math

import jax
import jax.numpy as jnp
from jax import lax
from jax.experimental import pallas as pl
from jax.experimental.pallas import tpu as pltpu
from jax.sharding import PartitionSpec as P

SWEEPS = 4
UNROLL = 16
GROUPS = 4
EARLY = 5
AHEAD = 2
LANES = 128
WIDTH = 128
FOLD_LIMIT = 2.0 ** 60
C1 = 2.0 * math.sqrt(2.0 / math.pi)
C3 = 8.0 * math.sqrt(2.0 / math.pi) * 0.044715
F32, BF16 = jnp.float32, jnp.bfloat16
MESH = pl.DeviceIdType.MESH
CONTRACT0 = (((0,), (0,)), ((), ()))


def offsets(n):
    return sorted(range(1, n), key=lambda i: (abs(2 * i - n), i))


def signal_all(n, me):
    barrier = pltpu.get_barrier_semaphore()
    for i in offsets(n):
        pl.semaphore_signal(barrier, inc=1, device_id={"time": lax.rem(me + i, n)}, device_id_type=MESH)


def wait_bytes(ref, *sems):
    for sem in sems:
        pltpu.make_async_copy(ref, ref, sem).wait()


def one_hot(cond):
    return jnp.where(cond, 1.0, 0.0).astype(BF16)


def share_parameters(n, me, scale, shift, step, mine, mine_step, mods, steps, send_sem, recv_sem):
    per = scale.shape[0]
    mine[0:per] = scale[...]
    mine[per:2 * per] = shift[...]
    lane = lax.broadcasted_iota(jnp.int32, (1, LANES), 1)
    row = jnp.zeros((1, LANES), F32)
    for i in range(per):
        row = jnp.where(lane == i, step[i], row)
    mine_step[...] = row
    mods[me] = mine[...]
    steps[me] = mine_step[...]
    pl.semaphore_wait(pltpu.get_barrier_semaphore(), n - 1)
    size = n // GROUPS
    for i in offsets(n):
        q = lax.rem(me + i, n)
        group = lax.rem(me // size - q // size + GROUPS, GROUPS)
        pltpu.make_async_remote_copy(
            mine, mods.at[me], send_sem.at[0], recv_sem.at[group], device_id={"time": q}, device_id_type=MESH).start()
    for i in offsets(n):
        pltpu.make_async_remote_copy(
            mine_step, steps.at[me], send_sem.at[1], recv_sem.at[GROUPS],
            device_id={"time": lax.rem(me + i, n)}, device_id_type=MESH).start()


def transposed(parts):
    rows = jnp.concatenate(parts, axis=0)
    if rows.shape[0] < LANES:
        rows = jnp.concatenate([rows, jnp.zeros((LANES - rows.shape[0], rows.shape[1]), F32)], axis=0)
    return rows.T.astype(BF16)


def scale_row(j, per):
    return j // per * (2 * per) + lax.rem(j, per)


def run_sweeps(n, per, fold, me, get_mods, w_in, w_out_t, ready, step_ref, out_ref, x_scr, w_scr, xs_scr, z_scr, h_scr, res_scr, send_sem, recv_sem):
    chunks, chans, width = x_scr.shape
    tokens = res_scr.shape[3]
    cuts = tokens // width
    share = chunks // cuts
    steps = n * per
    tiles = steps // 2
    half_lanes = LANES // 2

    row = lax.broadcasted_iota(jnp.int32, (LANES, LANES), 0)
    x_first = x_scr[0].astype(BF16)

    @pl.loop(0, steps)
    def _(j):
        xs_scr[j] = x_first

    h_scr[...] = jnp.zeros_like(h_scr)
    lane = lax.broadcasted_iota(jnp.int32, (1, LANES), 1)
    slot = lax.rem(lane, half_lanes)
    spread = one_hot((lax.rem(lane, chans) == row) & (slot < 3 * chans))
    w3 = 0.5 * lax.dot_general(w_in, spread[:chans], CONTRACT0, preferred_element_type=F32)
    wide_row = lax.broadcasted_iota(jnp.int32, (LANES, 2 * LANES), 0)
    wide_lane = lax.broadcasted_iota(jnp.int32, (1, 2 * LANES), 1)

    if fold:
        fixed = jnp.where(slot < chans, w3, 0.0)
        w3 = w3 + jnp.where(slot == 3 * chans, 0.5, 0.0)
        low_lanes = (slot >= 2 * chans) & (slot < 3 * chans)
        wide_slot = lax.rem(wide_lane, half_lanes)
        source = scale_row(wide_lane // half_lanes, per) + jnp.where(wide_slot == 3 * chans, per, 0)
        source = jnp.where((wide_slot >= chans) & (wide_slot <= 3 * chans), source, -8 * steps)
        picks = [one_hot(wide_row - 8 * t == source) for t in range(n // GROUPS * per // 4)]
        for k in range(GROUPS):
            first, mods_t = get_mods(k)
            picked = [jnp.dot(mods_t, pick, preferred_element_type=F32) for pick in picks]
            for t in range(2 * len(picks)):
                mod = picked[t // 2][:, t % 2 * LANES:(t % 2 + 1) * LANES]
                prod = w3 * mod + fixed
                rest = prod - jnp.where(low_lanes, prod.astype(BF16).astype(F32), 0.0)
                w_scr[first * per // 2 + t] = rest.astype(BF16)
    else:
        mods_t = get_mods()
        w_scr[0] = (w3 * jnp.where(lane < chans, 2.0, 0.0)).astype(BF16)

    ones_rows = jnp.ones((chans, width), BF16)
    zero_rows = jnp.zeros((half_lanes, width), BF16)
    unroll = UNROLL if fold else 2 * AHEAD
    groups = tiles // unroll
    per_chunk = SWEEPS * groups
    early = max(unroll - EARLY, 0)

    def half_pre(t, x):
        tops = [jnp.concatenate([x[p], x[p], x[p], ones_rows], axis=0) for p in range(2)]
        if fold:
            left = jnp.concatenate([tops[0], zero_rows], axis=0)
            right = jnp.concatenate([zero_rows, tops[1]], axis=0)
            return jnp.dot(w_scr[t], jnp.concatenate([left, right], axis=1), preferred_element_type=F32)
        rhs = jnp.concatenate([jnp.concatenate([top, zero_rows], axis=0) for top in tops], axis=1)
        pre = jnp.dot(w_scr[0], rhs, preferred_element_type=F32)
        src = scale_row(2 * t + wide_lane // width, per)
        scale = jnp.dot(mods_t, one_hot(wide_row == src), preferred_element_type=F32)
        shift = jnp.dot(mods_t, one_hot(wide_row == src + per), preferred_element_type=F32)
        return 0.5 * (pre * (1.0 + scale) + shift)

    def project(hidden):
        return jnp.dot(w_out_t, hidden, preferred_element_type=F32)

    def load_xs(t):
        return xs_scr[2 * t], xs_scr[2 * t + 1]

    def advance(g, t, d, d_prev, total, first=None):
        c = jnp.maximum(g, 0) // per_chunk
        lanes = pl.ds(pl.multiple_of(lax.rem(c, cuts) * width, width), width)
        x0 = x_scr[c]
        x_next = x_scr[jnp.minimum((g + per_chunk) // per_chunk, chunks - 1)]
        last = lax.rem(g + per_chunk, per_chunk) >= per_chunk - groups
        for p in range(2):
            j = 2 * t + p
            i = jnp.maximum(j - 1, 0)
            part = d[:, p * width:(p + 1) * width]
            total = total + (0.5 * step_ref[i // per, 0, lax.rem(i, per)]) * (d_prev + part)
            if p == 0 and first is not None:
                total = jnp.where(first, x0, total)
            xs_scr[j] = jnp.where(last, x_next, total).astype(BF16)
            res_scr[j, c // cuts, :, lanes] = total
            d_prev = part
        return d_prev, total

    def send(b, cut=None):
        lanes = slice(None) if cut is None else pl.ds(cut * width, width)
        place = (slice(None), me * share + b, slice(None), lanes)
        for i in offsets(n):
            q = lax.rem(me + i, n)
            pltpu.make_async_remote_copy(
                res_scr.at[pl.ds(q * per, per), b, :, lanes], out_ref.at[place], send_sem, recv_sem,
                device_id={"time": q}, device_id_type=MESH).start()
        out_ref[place] = res_scr[pl.ds(me * per, per), b, :, lanes]

    def body(g, carry):
        t0 = lax.rem(g, groups) * unroll
        t_next = lax.rem(g + 1, groups) * unroll
        xs = [load_xs(t0 + u) for u in range(AHEAD, unroll)] + [load_xs(t_next + u) for u in range(AHEAD)]
        ds = [project(h_scr[...])]
        halves = {u: z_scr[u] for u in range(AHEAD)}
        for u in range(unroll):
            v = u + AHEAD
            if v < unroll:
                halves[v] = half_pre(t0 + v, xs[u])
            half = halves.pop(u)
            arg = half * (half * half * C3 + C1)
            hidden = (half * (1.0 + jnp.tanh(arg))).astype(BF16)
            if early <= u < early + AHEAD:
                z_scr[u - early] = half_pre(t_next + u - early, xs[u - early - AHEAD])
            if u < unroll - 1:
                ds.append(project(hidden))
            else:
                h_scr[...] = hidden
        carry = advance(g - 1, lax.rem(t0 + tiles - 1, tiles), ds[0], *carry)
        for u in range(unroll - 1):
            carry = advance(g, t0 + u, ds[u + 1], *carry, first=t0 == 0 if u == 0 else None)

        for c in range(cuts, chunks):
            if c % cuts == 0 or c > chunks - cuts:
                @pl.when(g == c * per_chunk)
                def _(c=c):
                    send((c - 1) // cuts, None if c % cuts == 0 else (c - 1) % cuts)

        return carry

    for u in range(AHEAD):
        z_scr[u] = half_pre(u, (x_first, x_first))
    zero = jnp.zeros((chans, width), F32)
    total_groups = chunks * per_chunk
    ready()
    carry = lax.fori_loop(0, total_groups, body, (zero, x_scr[0]))
    advance(total_groups - 1, tiles - 1, project(h_scr[...]), *carry)
    send(share - 1, cuts - 1)
    wait_bytes(res_scr.at[pl.ds(0, (n - 1) * per)], recv_sem, send_sem)


def x_loads(me, x_hbm, x_scr, sem):
    chunks, _, width = x_scr.shape
    cuts = x_hbm.shape[2] // width
    return [
        pltpu.make_async_copy(
            x_hbm.at[me * (chunks // cuts) + c // cuts, :, pl.ds(c % cuts * width, width)], x_scr.at[c], sem.at[c])
        for c in range(chunks)
    ]


def folded_kernel(n, x_hbm, scale_hbm, shift_hbm, step_hbm, w_in_hbm, w_out_hbm, out_ref, mods, steps_ref, flag_ref, scale, shift, step, w_in, w_out_t, mine, mine_step, step_all, load_sem, x_sem, param_send, param_recv, x_scr, w_scr, xs_scr, z_scr, h_scr, res_scr, send_sem, recv_sem):
    me = lax.axis_index("time")
    per = scale.shape[0]
    loads = [
        pltpu.make_async_copy(src, dst, load_sem.at[k])
        for k, (src, dst) in enumerate((
            (scale_hbm, scale), (shift_hbm, shift), (step_hbm, step), (w_in_hbm, w_in), (w_out_hbm, w_out_t)))
    ] + x_loads(me, x_hbm, x_scr, x_sem)
    for load in loads:
        load.start()
    signal_all(n, me)
    for load in loads:
        load.wait()
    share_parameters(n, me, scale, shift, step, mine, mine_step, mods, steps_ref, param_send, param_recv)

    tops = []

    def get_mods(k):
        size = n // GROUPS
        wait_bytes(mods.at[pl.ds(0, size if k else size - 1)], param_recv.at[k])
        first = lax.rem(me // size + k, GROUPS) * size
        parts = [mods[first + q].astype(F32) for q in range(size)]
        tops.extend(jnp.abs(1.0 + part[:per]) for part in parts)
        return first, transposed(parts)

    def ready():
        top = functools.reduce(jnp.maximum, tops)
        flag_ref[0] = (jnp.max(top) * jnp.max(jnp.abs(w_in[...].astype(F32))) <= FOLD_LIMIT).astype(jnp.int32)
        wait_bytes(steps_ref.at[pl.ds(0, n - 1)], param_recv.at[GROUPS], param_send.at[1])
        wait_bytes(mods.at[pl.ds(0, n - 1)], param_send.at[0])
        to_scalars = pltpu.make_async_copy(steps_ref, step_all, load_sem.at[0])
        to_scalars.start()
        to_scalars.wait()

    run_sweeps(n, per, True, me, get_mods, w_in[...], w_out_t[...], ready, step_all, out_ref, x_scr, w_scr, xs_scr, z_scr, h_scr, res_scr, send_sem, recv_sem)


def wide_kernel(n, per, x_hbm, mods, w_in_ref, w_out_ref, step_ref, out_ref, x_sem, x_scr, w_scr, xs_scr, z_scr, h_scr, res_scr, send_sem, recv_sem):
    me = lax.axis_index("time")
    loads = x_loads(me, x_hbm, x_scr, x_sem)
    for load in loads:
        load.start()
    signal_all(n, me)
    for load in loads:
        load.wait()

    def ready():
        pl.semaphore_wait(pltpu.get_barrier_semaphore(), n - 1)

    run_sweeps(n, per, False, me, lambda: transposed([mods[q].astype(F32) for q in range(n)]), w_in_ref[...], w_out_ref[...], ready, step_ref, out_ref, x_scr, w_scr, xs_scr, z_scr, h_scr, res_scr, send_sem, recv_sem)


def solution(mesh):
    n = mesh.shape["time"]
    vmem = pl.BlockSpec(memory_space=pltpu.VMEM)
    smem = pl.BlockSpec(memory_space=pltpu.SMEM)

    def local(x_init, w_in, w_out, mod_scale, mod_shift, step_size):
        batch, tokens, chans = x_init.shape
        per, hidden = mod_scale.shape
        share = batch // n
        any_spec = pl.BlockSpec(memory_space=pl.ANY)
        steps = n * per
        chunks = share * tokens // WIDTH
        x_t = jnp.swapaxes(x_init, 1, 2)
        out_type = jax.ShapeDtypeStruct((per, batch, chans, tokens), F32)
        dma = pltpu.SemaphoreType.DMA

        def scratch(folded):
            return [
                pltpu.VMEM((chunks, chans, WIDTH), F32),
                pltpu.VMEM((steps // 2 if folded else 1, hidden, LANES), BF16),
                pltpu.VMEM((steps, chans, WIDTH), BF16),
                pltpu.VMEM((AHEAD, hidden, 2 * WIDTH), F32),
                pltpu.VMEM((hidden, 2 * WIDTH), BF16),
                pltpu.VMEM((steps, share, chans, tokens), F32),
                dma,
                dma,
            ]

        out, mods, step_all, flag = pl.pallas_call(
            functools.partial(folded_kernel, n),
            out_shape=(
                out_type,
                jax.ShapeDtypeStruct((n, 2 * per, hidden), BF16),
                jax.ShapeDtypeStruct((n, 1, LANES), F32),
                jax.ShapeDtypeStruct((1,), jnp.int32),
            ),
            in_specs=[any_spec] * 6,
            out_specs=(vmem, vmem, vmem, smem),
            scratch_shapes=[
                pltpu.VMEM((per, hidden), BF16),
                pltpu.VMEM((per, hidden), BF16),
                pltpu.SMEM((per,), F32),
                pltpu.VMEM((chans, hidden), BF16),
                pltpu.VMEM((chans, hidden), BF16),
                pltpu.VMEM((2 * per, hidden), BF16),
                pltpu.VMEM((1, LANES), F32),
                pltpu.SMEM((n, 1, LANES), F32),
                dma((5,)),
                dma((chunks,)),
                dma((2,)),
                dma((GROUPS + 1,)),
            ] + scratch(True),
            compiler_params=pltpu.CompilerParams(collective_id=0, has_side_effects=True, vmem_limit_bytes=56 * 1024 * 1024),
            name="folded",
        )(x_t, mod_scale, mod_shift, step_size, w_in, w_out.T)

        def wide(out, mods, step_all):
            return pl.pallas_call(
                functools.partial(wide_kernel, n, per),
                out_shape=out_type,
                in_specs=[any_spec] + [vmem] * 3 + [smem],
                out_specs=vmem,
                scratch_shapes=[dma((chunks,))] + scratch(False),
                compiler_params=pltpu.CompilerParams(collective_id=1, has_side_effects=True, vmem_limit_bytes=40 * 1024 * 1024),
                name="wide",
            )(x_t, mods, w_in, w_out.T, step_all)

        out = lax.cond(flag[0] != 0, lambda out, *rest: out, wide, out, mods, step_all)
        return jnp.swapaxes(out, 2, 3)

    return jax.shard_map(local, mesh=mesh, in_specs=(P("data"), P(), P(), P("time"), P("time"), P("time")), out_specs=P("time", "data"), check_vma=False)
```

```python
import functools
import math

import jax
import jax.numpy as jnp
from jax import lax
from jax.experimental import pallas as pl
from jax.experimental.pallas import tpu as pltpu
from jax.sharding import PartitionSpec as P

SWEEPS = 4
UNROLL = 16
GROUPS = 4
EARLY = 5
AHEAD = 2
LANES = 128
WIDTH = 128
FOLD_LIMIT = 2.0 ** 60
C1 = 2.0 * math.sqrt(2.0 / math.pi)
C3 = 8.0 * math.sqrt(2.0 / math.pi) * 0.044715
F32, BF16 = jnp.float32, jnp.bfloat16
MESH = pl.DeviceIdType.MESH
CONTRACT0 = (((0,), (0,)), ((), ()))


def offsets(n):
    return sorted(range(1, n), key=lambda i: (abs(2 * i - n), i))


def signal_all(n, me):
    barrier = pltpu.get_barrier_semaphore()
    for i in offsets(n):
        pl.semaphore_signal(barrier, inc=1, device_id={"time": lax.rem(me + i, n)}, device_id_type=MESH)


def wait_bytes(ref, *sems):
    for sem in sems:
        pltpu.make_async_copy(ref, ref, sem).wait()


def one_hot(cond):
    return jnp.where(cond, 1.0, 0.0).astype(BF16)


def share_parameters(n, me, scale, shift, step, mine, mine_step, mods, steps, send_sem, recv_sem):
    per = scale.shape[0]
    mine[0:per] = scale[...]
    mine[per:2 * per] = shift[...]
    lane = lax.broadcasted_iota(jnp.int32, (1, LANES), 1)
    row = jnp.zeros((1, LANES), F32)
    for i in range(per):
        row = jnp.where(lane == i, step[i], row)
    mine_step[...] = row
    mods[me] = mine[...]
    steps[me] = mine_step[...]
    pl.semaphore_wait(pltpu.get_barrier_semaphore(), n - 1)
    size = n // GROUPS
    for i in offsets(n):
        q = lax.rem(me + i, n)
        group = lax.rem(me // size - q // size + GROUPS, GROUPS)
        pltpu.make_async_remote_copy(
            mine, mods.at[me], send_sem.at[0], recv_sem.at[group], device_id={"time": q}, device_id_type=MESH).start()
    for i in offsets(n):
        pltpu.make_async_remote_copy(
            mine_step, steps.at[me], send_sem.at[1], recv_sem.at[GROUPS],
            device_id={"time": lax.rem(me + i, n)}, device_id_type=MESH).start()


def transposed(parts):
    rows = jnp.concatenate(parts, axis=0)
    if rows.shape[0] < LANES:
        rows = jnp.concatenate([rows, jnp.zeros((LANES - rows.shape[0], rows.shape[1]), F32)], axis=0)
    return rows.T.astype(BF16)


def scale_row(j, per):
    return j // per * (2 * per) + lax.rem(j, per)


def run_sweeps(n, per, fold, me, get_mods, w_in, w_out_t, ready, step_ref, out_ref, x_scr, w_scr, xs_scr, z_scr, h_scr, res_scr, send_sem, recv_sem):
    chunks, chans, width = x_scr.shape
    tokens = res_scr.shape[3]
    cuts = tokens // width
    share = chunks // cuts
    steps = n * per
    tiles = steps // 2
    half_lanes = LANES // 2

    row = lax.broadcasted_iota(jnp.int32, (LANES, LANES), 0)
    x_first = x_scr[0].astype(BF16)

    @pl.loop(0, steps)
    def _(j):
        xs_scr[j] = x_first

    h_scr[...] = jnp.zeros_like(h_scr)
    lane = lax.broadcasted_iota(jnp.int32, (1, LANES), 1)
    slot = lax.rem(lane, half_lanes)
    spread = one_hot((lax.rem(lane, chans) == row) & (slot < 3 * chans))
    w3 = 0.5 * lax.dot_general(w_in, spread[:chans], CONTRACT0, preferred_element_type=F32)
    wide_row = lax.broadcasted_iota(jnp.int32, (LANES, 2 * LANES), 0)
    wide_lane = lax.broadcasted_iota(jnp.int32, (1, 2 * LANES), 1)

    if fold:
        fixed = jnp.where(slot < chans, w3, 0.0)
        w3 = w3 + jnp.where(slot == 3 * chans, 0.5, 0.0)
        low_lanes = (slot >= 2 * chans) & (slot < 3 * chans)
        wide_slot = lax.rem(wide_lane, half_lanes)
        source = scale_row(wide_lane // half_lanes, per) + jnp.where(wide_slot == 3 * chans, per, 0)
        source = jnp.where((wide_slot >= chans) & (wide_slot <= 3 * chans), source, -8 * steps)
        picks = [one_hot(wide_row - 8 * t == source) for t in range(n // GROUPS * per // 4)]
        for k in sorted(range(GROUPS), key=lambda k: min(k, GROUPS - k)):
            first, mods_t = get_mods(k)
            picked = [jnp.dot(mods_t, pick, preferred_element_type=F32) for pick in picks]
            for t in range(2 * len(picks)):
                mod = picked[t // 2][:, t % 2 * LANES:(t % 2 + 1) * LANES]
                prod = w3 * mod + fixed
                rest = prod - jnp.where(low_lanes, prod.astype(BF16).astype(F32), 0.0)
                w_scr[first * per // 2 + t] = rest.astype(BF16)
    else:
        mods_t = get_mods()
        w_scr[0] = (w3 * jnp.where(lane < chans, 2.0, 0.0)).astype(BF16)

    ones_rows = jnp.ones((chans, width), BF16)
    zero_rows = jnp.zeros((half_lanes, width), BF16)
    unroll = UNROLL if fold else 2 * AHEAD
    groups = tiles // unroll
    per_chunk = SWEEPS * groups
    early = max(unroll - EARLY, 0)

    def half_pre(t, x):
        tops = [jnp.concatenate([x[p], x[p], x[p], ones_rows], axis=0) for p in range(2)]
        if fold:
            left = jnp.concatenate([tops[0], zero_rows], axis=0)
            right = jnp.concatenate([zero_rows, tops[1]], axis=0)
            return jnp.dot(w_scr[t], jnp.concatenate([left, right], axis=1), preferred_element_type=F32)
        rhs = jnp.concatenate([jnp.concatenate([top, zero_rows], axis=0) for top in tops], axis=1)
        pre = jnp.dot(w_scr[0], rhs, preferred_element_type=F32)
        src = scale_row(2 * t + wide_lane // width, per)
        scale = jnp.dot(mods_t, one_hot(wide_row == src), preferred_element_type=F32)
        shift = jnp.dot(mods_t, one_hot(wide_row == src + per), preferred_element_type=F32)
        return 0.5 * (pre * (1.0 + scale) + shift)

    def project(hidden):
        return jnp.dot(w_out_t, hidden, preferred_element_type=F32)

    def load_xs(t):
        return xs_scr[2 * t], xs_scr[2 * t + 1]

    def advance(g, t, d, d_prev, total, first=None):
        c = jnp.maximum(g, 0) // per_chunk
        lanes = pl.ds(pl.multiple_of(lax.rem(c, cuts) * width, width), width)
        x0 = x_scr[c]
        x_next = x_scr[jnp.minimum((g + per_chunk) // per_chunk, chunks - 1)]
        last = lax.rem(g + per_chunk, per_chunk) >= per_chunk - groups
        for p in range(2):
            j = 2 * t + p
            i = jnp.maximum(j - 1, 0)
            part = d[:, p * width:(p + 1) * width]
            total = total + (0.5 * step_ref[i // per, 0, lax.rem(i, per)]) * (d_prev + part)
            if p == 0 and first is not None:
                total = jnp.where(first, x0, total)
            xs_scr[j] = jnp.where(last, x_next, total).astype(BF16)
            res_scr[j, c // cuts, :, lanes] = total
            d_prev = part
        return d_prev, total

    def send(b, cut=None):
        lanes = slice(None) if cut is None else pl.ds(cut * width, width)
        place = (slice(None), me * share + b, slice(None), lanes)
        for i in offsets(n):
            q = lax.rem(me + i, n)
            pltpu.make_async_remote_copy(
                res_scr.at[pl.ds(q * per, per), b, :, lanes], out_ref.at[place], send_sem, recv_sem,
                device_id={"time": q}, device_id_type=MESH).start()
        out_ref[place] = res_scr[pl.ds(me * per, per), b, :, lanes]

    def body(g, carry):
        t0 = lax.rem(g, groups) * unroll
        t_next = lax.rem(g + 1, groups) * unroll
        xs = [load_xs(t0 + u) for u in range(AHEAD, unroll)] + [load_xs(t_next + u) for u in range(AHEAD)]
        ds = [project(h_scr[...])]
        halves = {u: z_scr[u] for u in range(AHEAD)}
        for u in range(unroll):
            v = u + AHEAD
            if v < unroll:
                halves[v] = half_pre(t0 + v, xs[u])
            half = halves.pop(u)
            arg = half * (half * half * C3 + C1)
            hidden = (half * (1.0 + jnp.tanh(arg))).astype(BF16)
            if early <= u < early + AHEAD:
                z_scr[u - early] = half_pre(t_next + u - early, xs[u - early - AHEAD])
            if u < unroll - 1:
                ds.append(project(hidden))
            else:
                h_scr[...] = hidden
        carry = advance(g - 1, lax.rem(t0 + tiles - 1, tiles), ds[0], *carry)
        for u in range(unroll - 1):
            carry = advance(g, t0 + u, ds[u + 1], *carry, first=t0 == 0 if u == 0 else None)

        for c in range(cuts, chunks):
            if c % cuts == 0 or c > chunks - cuts:
                @pl.when(g == c * per_chunk)
                def _(c=c):
                    send((c - 1) // cuts, None if c % cuts == 0 else (c - 1) % cuts)

        return carry

    for u in range(AHEAD):
        z_scr[u] = half_pre(u, (x_first, x_first))
    zero = jnp.zeros((chans, width), F32)
    total_groups = chunks * per_chunk
    ready()
    carry = lax.fori_loop(0, total_groups, body, (zero, x_scr[0]))
    advance(total_groups - 1, tiles - 1, project(h_scr[...]), *carry)
    send(share - 1, cuts - 1)
    wait_bytes(res_scr.at[pl.ds(0, (n - 1) * per)], recv_sem, send_sem)


def x_loads(me, x_hbm, x_scr, sem):
    chunks, _, width = x_scr.shape
    cuts = x_hbm.shape[2] // width
    return [
        pltpu.make_async_copy(
            x_hbm.at[me * (chunks // cuts) + c // cuts, :, pl.ds(c % cuts * width, width)], x_scr.at[c], sem.at[c])
        for c in range(chunks)
    ]


def folded_kernel(n, x_hbm, scale_hbm, shift_hbm, step_hbm, w_in_hbm, w_out_hbm, out_ref, mods, steps_ref, flag_hbm, scale, shift, step, w_in, w_out_t, mine, mine_step, step_all, flag, load_sem, x_sem, param_send, param_recv, x_scr, w_scr, xs_scr, z_scr, h_scr, res_scr, send_sem, recv_sem):
    me = lax.axis_index("time")
    per = scale.shape[0]
    loads = [
        pltpu.make_async_copy(src, dst, load_sem.at[k])
        for k, (src, dst) in enumerate((
            (scale_hbm, scale), (shift_hbm, shift), (step_hbm, step), (w_in_hbm, w_in), (w_out_hbm, w_out_t)))
    ] + x_loads(me, x_hbm, x_scr, x_sem)
    for load in loads:
        load.start()
    signal_all(n, me)
    for load in loads:
        load.wait()
    share_parameters(n, me, scale, shift, step, mine, mine_step, mods, steps_ref, param_send, param_recv)

    tops = []
    flag_copy = pltpu.make_async_copy(flag, flag_hbm, load_sem.at[1])

    def get_mods(k):
        size = n // GROUPS
        wait_bytes(mods.at[pl.ds(0, size if k else size - 1)], param_recv.at[k])
        first = lax.rem(me // size + k, GROUPS) * size
        parts = [mods[first + q].astype(F32) for q in range(size)]
        tops.extend(jnp.abs(1.0 + part[:per]) for part in parts)
        return first, transposed(parts)

    def ready():
        top = functools.reduce(jnp.maximum, tops)
        flag[0] = (jnp.max(top) * jnp.max(jnp.abs(w_in[...].astype(F32))) <= FOLD_LIMIT).astype(jnp.int32)
        flag_copy.start()
        wait_bytes(steps_ref.at[pl.ds(0, n - 1)], param_recv.at[GROUPS], param_send.at[1])
        wait_bytes(mods.at[pl.ds(0, n - 1)], param_send.at[0])
        to_scalars = pltpu.make_async_copy(steps_ref, step_all, load_sem.at[0])
        to_scalars.start()
        to_scalars.wait()

    run_sweeps(n, per, True, me, get_mods, w_in[...], w_out_t[...], ready, step_all, out_ref, x_scr, w_scr, xs_scr, z_scr, h_scr, res_scr, send_sem, recv_sem)
    flag_copy.wait()


def wide_kernel(n, per, x_hbm, mods, w_in_ref, w_out_ref, step_ref, out_ref, x_sem, x_scr, w_scr, xs_scr, z_scr, h_scr, res_scr, send_sem, recv_sem):
    me = lax.axis_index("time")
    loads = x_loads(me, x_hbm, x_scr, x_sem)
    for load in loads:
        load.start()
    signal_all(n, me)
    for load in loads:
        load.wait()

    def ready():
        pl.semaphore_wait(pltpu.get_barrier_semaphore(), n - 1)

    run_sweeps(n, per, False, me, lambda: transposed([mods[q].astype(F32) for q in range(n)]), w_in_ref[...], w_out_ref[...], ready, step_ref, out_ref, x_scr, w_scr, xs_scr, z_scr, h_scr, res_scr, send_sem, recv_sem)


def solution(mesh):
    n = mesh.shape["time"]
    vmem = pl.BlockSpec(memory_space=pltpu.VMEM)
    smem = pl.BlockSpec(memory_space=pltpu.SMEM)

    def local(x_init, w_in, w_out, mod_scale, mod_shift, step_size):
        batch, tokens, chans = x_init.shape
        per, hidden = mod_scale.shape
        share = batch // n
        any_spec = pl.BlockSpec(memory_space=pl.ANY)
        steps = n * per
        chunks = share * tokens // WIDTH
        x_t = jnp.swapaxes(x_init, 1, 2)
        out_type = jax.ShapeDtypeStruct((per, batch, chans, tokens), F32)
        dma = pltpu.SemaphoreType.DMA

        def scratch(folded):
            return [
                pltpu.VMEM((chunks, chans, WIDTH), F32),
                pltpu.VMEM((steps // 2 if folded else 1, hidden, LANES), BF16),
                pltpu.VMEM((steps, chans, WIDTH), BF16),
                pltpu.VMEM((AHEAD, hidden, 2 * WIDTH), F32),
                pltpu.VMEM((hidden, 2 * WIDTH), BF16),
                pltpu.VMEM((steps, share, chans, tokens), F32),
                dma,
                dma,
            ]

        out, mods, step_all, flag = pl.pallas_call(
            functools.partial(folded_kernel, n),
            out_shape=(
                out_type,
                jax.ShapeDtypeStruct((n, 2 * per, hidden), BF16),
                jax.ShapeDtypeStruct((n, 1, LANES), F32),
                jax.ShapeDtypeStruct((1,), jnp.int32),
            ),
            in_specs=[any_spec] * 6,
            out_specs=(vmem, vmem, vmem, any_spec),
            scratch_shapes=[
                pltpu.VMEM((per, hidden), BF16),
                pltpu.VMEM((per, hidden), BF16),
                pltpu.SMEM((per,), F32),
                pltpu.VMEM((chans, hidden), BF16),
                pltpu.VMEM((chans, hidden), BF16),
                pltpu.VMEM((2 * per, hidden), BF16),
                pltpu.VMEM((1, LANES), F32),
                pltpu.SMEM((n, 1, LANES), F32),
                pltpu.SMEM((1,), jnp.int32),
                dma((5,)),
                dma((chunks,)),
                dma((2,)),
                dma((GROUPS + 1,)),
            ] + scratch(True),
            compiler_params=pltpu.CompilerParams(collective_id=0, has_side_effects=True, vmem_limit_bytes=56 * 1024 * 1024),
            name="folded",
        )(x_t, mod_scale, mod_shift, step_size, w_in, w_out.T)

        def wide(out, mods, step_all):
            return pl.pallas_call(
                functools.partial(wide_kernel, n, per),
                out_shape=out_type,
                in_specs=[any_spec] + [vmem] * 3 + [smem],
                out_specs=vmem,
                scratch_shapes=[dma((chunks,))] + scratch(False),
                compiler_params=pltpu.CompilerParams(collective_id=1, has_side_effects=True, vmem_limit_bytes=40 * 1024 * 1024),
                name="wide",
            )(x_t, mods, w_in, w_out.T, step_all)

        out = lax.cond(flag[0] != 0, lambda out, *rest: out, wide, out, mods, step_all)
        return jnp.swapaxes(out, 2, 3)

    return jax.shard_map(local, mesh=mesh, in_specs=(P("data"), P(), P(), P("time"), P("time"), P("time")), out_specs=P("time", "data"), check_vma=False)
```

```python
import functools
import math

import jax
import jax.numpy as jnp
from jax import lax
from jax.experimental import pallas as pl
from jax.experimental.pallas import tpu as pltpu
from jax.sharding import PartitionSpec as P

SWEEPS = 4
UNROLL = 16
GROUPS = 4
EARLY = 5
AHEAD = 2
LANES = 128
WIDTH = 128
FOLD_LIMIT = 2.0 ** 60
C1 = 2.0 * math.sqrt(2.0 / math.pi)
C3 = 8.0 * math.sqrt(2.0 / math.pi) * 0.044715
F32, BF16 = jnp.float32, jnp.bfloat16
MESH = pl.DeviceIdType.MESH
CONTRACT0 = (((0,), (0,)), ((), ()))


def offsets(n):
    return sorted(range(1, n), key=lambda i: (abs(2 * i - n), i))


def signal_all(n, me):
    barrier = pltpu.get_barrier_semaphore()
    for i in offsets(n):
        pl.semaphore_signal(barrier, inc=1, device_id={"time": lax.rem(me + i, n)}, device_id_type=MESH)


def wait_bytes(ref, *sems):
    for sem in sems:
        pltpu.make_async_copy(ref, ref, sem).wait()


def one_hot(cond):
    return jnp.where(cond, 1.0, 0.0).astype(BF16)


def share_parameters(n, me, scale, shift, step, mine, mine_step, mods, steps, send_sem, recv_sem):
    per = scale.shape[0]
    mine[0:per] = scale[...]
    mine[per:2 * per] = shift[...]
    for i in range(per):
        mine_step[i:i + 1] = jnp.full((1, LANES), 0.5 * step[i], F32)
    mods[me] = mine[...]
    steps[me] = mine_step[...]
    pl.semaphore_wait(pltpu.get_barrier_semaphore(), n - 1)
    size = n // GROUPS
    for i in offsets(n):
        q = lax.rem(me + i, n)
        group = lax.rem(me // size - q // size + GROUPS, GROUPS)
        pltpu.make_async_remote_copy(
            mine, mods.at[me], send_sem.at[0], recv_sem.at[group], device_id={"time": q}, device_id_type=MESH).start()
    for i in offsets(n):
        pltpu.make_async_remote_copy(
            mine_step, steps.at[me], send_sem.at[1], recv_sem.at[GROUPS],
            device_id={"time": lax.rem(me + i, n)}, device_id_type=MESH).start()


def transposed(parts):
    rows = jnp.concatenate(parts, axis=0)
    if rows.shape[0] < LANES:
        rows = jnp.concatenate([rows, jnp.zeros((LANES - rows.shape[0], rows.shape[1]), F32)], axis=0)
    return rows.T.astype(BF16)


def scale_row(j, per):
    return j // per * (2 * per) + lax.rem(j, per)


def run_sweeps(n, per, fold, me, get_mods, w_in, w_out_t, ready, step_ref, out_ref, x_scr, w_scr, xs_scr, z_scr, h_scr, res_scr, send_sem, recv_sem):
    chunks, chans, width = x_scr.shape
    tokens = res_scr.shape[3]
    cuts = tokens // width
    share = chunks // cuts
    steps = n * per
    tiles = steps // 2
    half_lanes = LANES // 2

    row = lax.broadcasted_iota(jnp.int32, (LANES, LANES), 0)
    x_first = x_scr[0].astype(BF16)

    @pl.loop(0, steps)
    def _(j):
        xs_scr[j] = x_first

    h_scr[...] = jnp.zeros_like(h_scr)
    lane = lax.broadcasted_iota(jnp.int32, (1, LANES), 1)
    slot = lax.rem(lane, half_lanes)
    spread = one_hot((lax.rem(lane, chans) == row) & (slot < 3 * chans))
    w3 = 0.5 * lax.dot_general(w_in, spread[:chans], CONTRACT0, preferred_element_type=F32)
    wide_row = lax.broadcasted_iota(jnp.int32, (LANES, 2 * LANES), 0)
    wide_lane = lax.broadcasted_iota(jnp.int32, (1, 2 * LANES), 1)

    if fold:
        fixed = jnp.where(slot < chans, w3, 0.0)
        w3 = w3 + jnp.where(slot == 3 * chans, 0.5, 0.0)
        low_lanes = (slot >= 2 * chans) & (slot < 3 * chans)
        wide_slot = lax.rem(wide_lane, half_lanes)
        source = scale_row(wide_lane // half_lanes, per) + jnp.where(wide_slot == 3 * chans, per, 0)
        source = jnp.where((wide_slot >= chans) & (wide_slot <= 3 * chans), source, -8 * steps)
        picks = [one_hot(wide_row - 8 * t == source) for t in range(n // GROUPS * per // 4)]
        for k in sorted(range(GROUPS), key=lambda k: min(k, GROUPS - k)):
            first, mods_t = get_mods(k)
            picked = [jnp.dot(mods_t, pick, preferred_element_type=F32) for pick in picks]
            for t in range(2 * len(picks)):
                mod = picked[t // 2][:, t % 2 * LANES:(t % 2 + 1) * LANES]
                prod = w3 * mod + fixed
                rest = prod - jnp.where(low_lanes, prod.astype(BF16).astype(F32), 0.0)
                w_scr[first * per // 2 + t] = rest.astype(BF16)
    else:
        mods_t = get_mods()
        w_scr[0] = (w3 * jnp.where(lane < chans, 2.0, 0.0)).astype(BF16)

    ones_rows = jnp.ones((chans, width), BF16)
    zero_rows = jnp.zeros((half_lanes, width), BF16)
    unroll = UNROLL if fold else 2 * AHEAD
    groups = tiles // unroll
    per_chunk = SWEEPS * groups
    early = max(unroll - EARLY, 0)

    def half_pre(t, x):
        tops = [jnp.concatenate([x[p], x[p], x[p], ones_rows], axis=0) for p in range(2)]
        if fold:
            left = jnp.concatenate([tops[0], zero_rows], axis=0)
            right = jnp.concatenate([zero_rows, tops[1]], axis=0)
            return jnp.dot(w_scr[t], jnp.concatenate([left, right], axis=1), preferred_element_type=F32)
        rhs = jnp.concatenate([jnp.concatenate([top, zero_rows], axis=0) for top in tops], axis=1)
        pre = jnp.dot(w_scr[0], rhs, preferred_element_type=F32)
        src = scale_row(2 * t + wide_lane // width, per)
        scale = jnp.dot(mods_t, one_hot(wide_row == src), preferred_element_type=F32)
        shift = jnp.dot(mods_t, one_hot(wide_row == src + per), preferred_element_type=F32)
        return 0.5 * (pre * (1.0 + scale) + shift)

    def project(hidden):
        return jnp.dot(w_out_t, hidden, preferred_element_type=F32)

    def load_xs(t):
        return xs_scr[2 * t], xs_scr[2 * t + 1]

    def advance(g, t, d, d_prev, total, first=None):
        c = jnp.maximum(g, 0) // per_chunk
        lanes = pl.ds(pl.multiple_of(lax.rem(c, cuts) * width, width), width)
        x0 = x_scr[c]
        x_next = x_scr[jnp.minimum((g + per_chunk) // per_chunk, chunks - 1)]
        last = lax.rem(g + per_chunk, per_chunk) >= per_chunk - groups
        for p in range(2):
            j = 2 * t + p
            i = jnp.maximum(j - 1, 0)
            part = d[:, p * width:(p + 1) * width]
            total = total + step_ref[i // per, pl.ds(lax.rem(i, per), 1)] * (d_prev + part)
            if p == 0 and first is not None:
                total = jnp.where(first, x0, total)
            xs_scr[j] = jnp.where(last, x_next, total).astype(BF16)
            res_scr[j, c // cuts, :, lanes] = total
            d_prev = part
        return d_prev, total

    def send(b, cut=None):
        lanes = slice(None) if cut is None else pl.ds(cut * width, width)
        place = (slice(None), me * share + b, slice(None), lanes)
        for i in offsets(n):
            q = lax.rem(me + i, n)
            pltpu.make_async_remote_copy(
                res_scr.at[pl.ds(q * per, per), b, :, lanes], out_ref.at[place], send_sem, recv_sem,
                device_id={"time": q}, device_id_type=MESH).start()
        out_ref[place] = res_scr[pl.ds(me * per, per), b, :, lanes]

    def body(g, carry):
        t0 = lax.rem(g, groups) * unroll
        t_next = lax.rem(g + 1, groups) * unroll
        xs = [load_xs(t0 + u) for u in range(AHEAD, unroll)] + [load_xs(t_next + u) for u in range(AHEAD)]
        ds = [project(h_scr[...])]
        halves = {u: z_scr[u] for u in range(AHEAD)}
        for u in range(unroll):
            v = u + AHEAD
            if v < unroll:
                halves[v] = half_pre(t0 + v, xs[u])
            half = halves.pop(u)
            arg = half * (half * half * C3 + C1)
            hidden = (half * (1.0 + jnp.tanh(arg))).astype(BF16)
            if early <= u < early + AHEAD:
                z_scr[u - early] = half_pre(t_next + u - early, xs[u - early - AHEAD])
            if u < unroll - 1:
                ds.append(project(hidden))
            else:
                h_scr[...] = hidden
        carry = advance(g - 1, lax.rem(t0 + tiles - 1, tiles), ds[0], *carry)
        for u in range(unroll - 1):
            carry = advance(g, t0 + u, ds[u + 1], *carry, first=t0 == 0 if u == 0 else None)

        for c in range(cuts, chunks):
            if c % cuts == 0 or c > chunks - cuts:
                @pl.when(g == c * per_chunk)
                def _(c=c):
                    send((c - 1) // cuts, None if c % cuts == 0 else (c - 1) % cuts)

        return carry

    for u in range(AHEAD):
        z_scr[u] = half_pre(u, (x_first, x_first))
    zero = jnp.zeros((chans, width), F32)
    total_groups = chunks * per_chunk
    ready()
    carry = lax.fori_loop(0, total_groups, body, (zero, x_scr[0]))
    advance(total_groups - 1, tiles - 1, project(h_scr[...]), *carry)
    send(share - 1, cuts - 1)
    wait_bytes(res_scr.at[pl.ds(0, (n - 1) * per)], recv_sem, send_sem)


def x_loads(me, x_hbm, x_scr, sem):
    chunks, _, width = x_scr.shape
    cuts = x_hbm.shape[2] // width
    return [
        pltpu.make_async_copy(
            x_hbm.at[me * (chunks // cuts) + c // cuts, :, pl.ds(c % cuts * width, width)], x_scr.at[c], sem.at[c])
        for c in range(chunks)
    ]


def folded_kernel(n, x_hbm, scale_hbm, shift_hbm, step_hbm, w_in_hbm, w_out_hbm, out_ref, mods, steps_ref, flag_hbm, scale, shift, step, w_in, w_out_t, mine, mine_step, flag, load_sem, x_sem, param_send, param_recv, x_scr, w_scr, xs_scr, z_scr, h_scr, res_scr, send_sem, recv_sem):
    me = lax.axis_index("time")
    per = scale.shape[0]
    loads = [
        pltpu.make_async_copy(src, dst, load_sem.at[k])
        for k, (src, dst) in enumerate((
            (scale_hbm, scale), (shift_hbm, shift), (step_hbm, step), (w_in_hbm, w_in), (w_out_hbm, w_out_t)))
    ] + x_loads(me, x_hbm, x_scr, x_sem)
    for load in loads:
        load.start()
    signal_all(n, me)
    for load in loads:
        load.wait()
    share_parameters(n, me, scale, shift, step, mine, mine_step, mods, steps_ref, param_send, param_recv)

    tops = []
    flag_copy = pltpu.make_async_copy(flag, flag_hbm, load_sem.at[1])

    def get_mods(k):
        size = n // GROUPS
        wait_bytes(mods.at[pl.ds(0, size if k else size - 1)], param_recv.at[k])
        first = lax.rem(me // size + k, GROUPS) * size
        parts = [mods[first + q].astype(F32) for q in range(size)]
        tops.extend(jnp.abs(1.0 + part[:per]) for part in parts)
        return first, transposed(parts)

    def ready():
        top = functools.reduce(jnp.maximum, tops)
        flag[0] = (jnp.max(top) * jnp.max(jnp.abs(w_in[...].astype(F32))) <= FOLD_LIMIT).astype(jnp.int32)
        flag_copy.start()
        wait_bytes(steps_ref.at[pl.ds(0, n - 1)], param_recv.at[GROUPS], param_send.at[1])
        wait_bytes(mods.at[pl.ds(0, n - 1)], param_send.at[0])

    run_sweeps(n, per, True, me, get_mods, w_in[...], w_out_t[...], ready, steps_ref, out_ref, x_scr, w_scr, xs_scr, z_scr, h_scr, res_scr, send_sem, recv_sem)
    flag_copy.wait()


def wide_kernel(n, per, x_hbm, mods, w_in_ref, w_out_ref, step_ref, out_ref, x_sem, x_scr, w_scr, xs_scr, z_scr, h_scr, res_scr, send_sem, recv_sem):
    me = lax.axis_index("time")
    loads = x_loads(me, x_hbm, x_scr, x_sem)
    for load in loads:
        load.start()
    signal_all(n, me)
    for load in loads:
        load.wait()

    def ready():
        pl.semaphore_wait(pltpu.get_barrier_semaphore(), n - 1)

    run_sweeps(n, per, False, me, lambda: transposed([mods[q].astype(F32) for q in range(n)]), w_in_ref[...], w_out_ref[...], ready, step_ref, out_ref, x_scr, w_scr, xs_scr, z_scr, h_scr, res_scr, send_sem, recv_sem)


def solution(mesh):
    n = mesh.shape["time"]
    vmem = pl.BlockSpec(memory_space=pltpu.VMEM)

    def local(x_init, w_in, w_out, mod_scale, mod_shift, step_size):
        batch, tokens, chans = x_init.shape
        per, hidden = mod_scale.shape
        share = batch // n
        any_spec = pl.BlockSpec(memory_space=pl.ANY)
        steps = n * per
        chunks = share * tokens // WIDTH
        x_t = jnp.swapaxes(x_init, 1, 2)
        out_type = jax.ShapeDtypeStruct((per, batch, chans, tokens), F32)
        dma = pltpu.SemaphoreType.DMA

        def scratch(folded):
            return [
                pltpu.VMEM((chunks, chans, WIDTH), F32),
                pltpu.VMEM((steps // 2 if folded else 1, hidden, LANES), BF16),
                pltpu.VMEM((steps, chans, WIDTH), BF16),
                pltpu.VMEM((AHEAD, hidden, 2 * WIDTH), F32),
                pltpu.VMEM((hidden, 2 * WIDTH), BF16),
                pltpu.VMEM((steps, share, chans, tokens), F32),
                dma,
                dma,
            ]

        out, mods, step_all, flag = pl.pallas_call(
            functools.partial(folded_kernel, n),
            out_shape=(
                out_type,
                jax.ShapeDtypeStruct((n, 2 * per, hidden), BF16),
                jax.ShapeDtypeStruct((n, per, LANES), F32),
                jax.ShapeDtypeStruct((1,), jnp.int32),
            ),
            in_specs=[any_spec] * 6,
            out_specs=(vmem, vmem, vmem, any_spec),
            scratch_shapes=[
                pltpu.VMEM((per, hidden), BF16),
                pltpu.VMEM((per, hidden), BF16),
                pltpu.SMEM((per,), F32),
                pltpu.VMEM((chans, hidden), BF16),
                pltpu.VMEM((chans, hidden), BF16),
                pltpu.VMEM((2 * per, hidden), BF16),
                pltpu.VMEM((per, LANES), F32),
                pltpu.SMEM((1,), jnp.int32),
                dma((5,)),
                dma((chunks,)),
                dma((2,)),
                dma((GROUPS + 1,)),
            ] + scratch(True),
            compiler_params=pltpu.CompilerParams(collective_id=0, has_side_effects=True, vmem_limit_bytes=56 * 1024 * 1024),
            name="folded",
        )(x_t, mod_scale, mod_shift, step_size, w_in, w_out.T)

        def wide(out, mods, step_all):
            return pl.pallas_call(
                functools.partial(wide_kernel, n, per),
                out_shape=out_type,
                in_specs=[any_spec] + [vmem] * 4,
                out_specs=vmem,
                scratch_shapes=[dma((chunks,))] + scratch(False),
                compiler_params=pltpu.CompilerParams(collective_id=1, has_side_effects=True, vmem_limit_bytes=40 * 1024 * 1024),
                name="wide",
            )(x_t, mods, w_in, w_out.T, step_all)

        out = lax.cond(flag[0] != 0, lambda out, *rest: out, wide, out, mods, step_all)
        return jnp.swapaxes(out, 2, 3)

    return jax.shard_map(local, mesh=mesh, in_specs=(P("data"), P(), P(), P("time"), P("time"), P("time")), out_specs=P("time", "data"), check_vma=False)
```
